128 devices in a mesh: dp: 1, tp: 2 (over core), ep: 64 (over z, y, x).
Axes of the slice: x: 4, y: 4, z: 4, core: 2. Of those that a mesh axis runs over, the one named last changes fastest.
Arguments:
- x: bfloat16 [64, 1024, 768], P(('dp', 'ep'))
- src_len: int32 [64], P(('dp', 'ep'))
- expert_idx: int32 [64, 1024, 2], P(('dp', 'ep'))
- ln_gain: float32 [4, 768], replicated
- ln_bias: float32 [4, 768], replicated
- w_query: bfloat16 [2, 768, 12, 64], P(None, None, 'tp')
- b_query: float32 [2, 12, 64], P(None, 'tp')
- w_key: bfloat16 [2, 768, 12, 64], P(None, None, 'tp')
- w_value: bfloat16 [2, 768, 12, 64], P(None, None, 'tp')
- b_value: float32 [2, 12, 64], P(None, 'tp')
- w_attn_out: bfloat16 [2, 12, 64, 768], P(None, 'tp')
- b_attn_out: float32 [2, 768], replicated
- w_fc1: bfloat16 [768, 3072], P(None, 'tp')
- b_fc1: float32 [3072], P('tp')
- w_fc2: bfloat16 [3072, 768], P('tp')
- b_fc2: float32 [768], replicated
- w_router: float32 [768, 128], replicated
- w_exp_in: bfloat16 [128, 768, 3072], P('ep', None, 'tp')
- b_exp_in: float32 [128, 3072], P('ep', 'tp')
- w_exp_out: bfloat16 [128, 3072, 768], P('ep', 'tp')
- b_exp_out: float32 [128, 768], P('ep')
Outputs:
- output: bfloat16 [64, 1024, 768], P(('dp', 'ep'))
All inputs are finite; a program needn't handle non-finite values.
Results may differ from the reference program's by a relative error of at most 0.0133347.
Values are sent between devices in bfloat16 or wider.
A program may use at most 1 GiB of HBM per device.

```python
import jax
import jax.numpy as jnp
from jax import lax

GROUPS = 64
ROWS_DEV = 1
SEQ_LEN = 1024
D_MODEL = 768
NUM_HEADS = 12
HEAD_DIM = 64
FF_DENSE = 3072
EXPERTS = 128
EXPERT_FF = 3072

BATCH = GROUPS * ROWS_DEV
TOKENS_GROUP = ROWS_DEV * SEQ_LEN
CAPACITY = 2 * ((TOKENS_GROUP + EXPERTS - 1) // EXPERTS)
DUMP_SLOT = EXPERTS * CAPACITY
INNER_DIM = NUM_HEADS * HEAD_DIM
LN_EPS = 1e-5


def layer_norm(hidden, gain, shift):
    hidden = hidden.astype(jnp.float32)
    centered = hidden - jnp.mean(hidden, axis=-1, keepdims=True)
    variance = jnp.mean(centered * centered, axis=-1, keepdims=True)
    return centered * lax.rsqrt(variance + LN_EPS) * gain + shift


def draw_routing(route_key):
    len_key, hot_key, pick_key, first_key, second_key = jax.random.split(route_key, 5)
    row_ids = jnp.arange(BATCH)
    lengths = jax.random.randint(len_key, (BATCH,), SEQ_LEN // 4, SEQ_LEN + 1)
    lengths = jnp.where(row_ids == 0, SEQ_LEN, lengths)
    lengths = jnp.where(row_ids == BATCH - 1, SEQ_LEN // 4, lengths)
    hot_count = max(EXPERTS // 16, 1)
    hot_start = jax.random.randint(hot_key, (), 0, EXPERTS)
    grid = (BATCH, SEQ_LEN)
    pick_hot = jax.random.randint(pick_key, grid, 0, 4) == 0
    uniform_first = jax.random.randint(first_key, grid, 0, EXPERTS)
    hot_first = (hot_start + uniform_first % hot_count) % EXPERTS
    first = jnp.where(pick_hot, hot_first, uniform_first)
    second = (first + jax.random.randint(second_key, grid, 1, EXPERTS)) % EXPERTS
    expert_idx = jnp.stack([first, second], axis=-1).astype(jnp.int32)
    return lengths.astype(jnp.int32), expert_idx


def scaled_normal(key, extent, scale):
    return jax.random.normal(key, extent, jnp.float32) * scale


def setup_inputs(seed: int = 0, part: int = 0) -> dict:
    part_key = jax.random.fold_in(jax.random.key(seed), part)
    x_key, route_key = jax.random.split(part_key, 2)
    keys = jax.random.split(jax.random.key(seed + 1), 18)
    src_len, expert_idx = draw_routing(route_key)
    attn_shape = (2, D_MODEL, NUM_HEADS, HEAD_DIM)
    model_scale = D_MODEL ** -0.5
    inner_scale = INNER_DIM ** -0.5
    return {
        'x': scaled_normal(x_key, (BATCH, SEQ_LEN, D_MODEL), 1.0).astype(jnp.bfloat16),
        'src_len': src_len,
        'expert_idx': expert_idx,
        'ln_gain': 1.0 + scaled_normal(keys[0], (4, D_MODEL), 0.2),
        'ln_bias': scaled_normal(keys[1], (4, D_MODEL), 0.2),
        'w_query': scaled_normal(keys[2], attn_shape, model_scale).astype(jnp.bfloat16),
        'b_query': scaled_normal(keys[3], (2, NUM_HEADS, HEAD_DIM), 0.5),
        'w_key': scaled_normal(keys[4], attn_shape, model_scale).astype(jnp.bfloat16),
        'w_value': scaled_normal(keys[5], attn_shape, model_scale).astype(jnp.bfloat16),
        'b_value': scaled_normal(keys[6], (2, NUM_HEADS, HEAD_DIM), 0.5),
        'w_attn_out': scaled_normal(keys[7], (2, NUM_HEADS, HEAD_DIM, D_MODEL), inner_scale).astype(jnp.bfloat16),
        'b_attn_out': scaled_normal(keys[8], (2, D_MODEL), 0.3),
        'w_fc1': scaled_normal(keys[9], (D_MODEL, FF_DENSE), model_scale).astype(jnp.bfloat16),
        'b_fc1': scaled_normal(keys[10], (FF_DENSE,), 0.5),
        'w_fc2': scaled_normal(keys[11], (FF_DENSE, D_MODEL), FF_DENSE ** -0.5).astype(jnp.bfloat16),
        'b_fc2': scaled_normal(keys[12], (D_MODEL,), 0.3),
        'w_router': scaled_normal(keys[13], (D_MODEL, EXPERTS), model_scale),
        'w_exp_in': scaled_normal(keys[14], (EXPERTS, D_MODEL, EXPERT_FF), model_scale).astype(jnp.bfloat16),
        'b_exp_in': scaled_normal(keys[15], (EXPERTS, EXPERT_FF), 0.5),
        'w_exp_out': scaled_normal(keys[16], (EXPERTS, EXPERT_FF, D_MODEL), EXPERT_FF ** -0.5).astype(jnp.bfloat16),
        'b_exp_out': scaled_normal(keys[17], (EXPERTS, D_MODEL), 0.5),
    }


def attention_row(residual, key_ok, gain, shift, w_q, b_q, w_k, w_v, b_v, w_o, b_o):
    normed = layer_norm(residual, gain, shift).astype(jnp.bfloat16)

    def project(weight):
        flat = jnp.dot(normed, weight.reshape(D_MODEL, INNER_DIM), preferred_element_type=jnp.float32)
        return flat.reshape(SEQ_LEN, NUM_HEADS, HEAD_DIM)

    query = (project(w_q) + b_q).astype(jnp.bfloat16)
    keys = project(w_k).astype(jnp.bfloat16)
    values = (project(w_v) + b_v).astype(jnp.bfloat16)
    scores = jnp.einsum('qhk,shk->hqs', query.astype(jnp.float32), keys.astype(jnp.float32)) * (HEAD_DIM ** -0.5)
    scores = jnp.where(key_ok[None, None, :], scores, -1e30)
    attn_probs = jax.nn.softmax(scores, axis=-1).astype(jnp.bfloat16)
    context = jnp.einsum('hqs,shk->qhk', attn_probs.astype(jnp.float32), values.astype(jnp.float32)).astype(jnp.bfloat16)
    projected = jnp.dot(context.reshape(SEQ_LEN, INNER_DIM), w_o.reshape(INNER_DIM, D_MODEL), preferred_element_type=jnp.float32)
    return (residual.astype(jnp.float32) + projected + b_o).astype(jnp.bfloat16)


def dense_ffn(residual, gain, shift, w_in, b_in, w_out, b_out):
    normed = layer_norm(residual, gain, shift).astype(jnp.bfloat16)
    inner = jax.nn.relu(jnp.dot(normed, w_in, preferred_element_type=jnp.float32) + b_in).astype(jnp.bfloat16)
    projected = jnp.dot(inner, w_out, preferred_element_type=jnp.float32)
    return (residual.astype(jnp.float32) + projected + b_out).astype(jnp.bfloat16)


def take_rows(rows, index):
    return rows[index]


def fill_table(dest_first, dest_second):
    token_ids = jnp.arange(TOKENS_GROUP, dtype=jnp.int32)
    table = jnp.full((DUMP_SLOT + 1,), TOKENS_GROUP, jnp.int32)
    table = table.at[dest_first].set(token_ids).at[dest_second].set(token_ids)
    return table[:DUMP_SLOT]


def run_expert(operands):
    rows_in, w_in, b_in, w_out, b_out = operands
    inner = jax.nn.relu(jnp.dot(rows_in, w_in, preferred_element_type=jnp.float32) + b_in).astype(jnp.bfloat16)
    return (jnp.dot(inner, w_out, preferred_element_type=jnp.float32) + b_out).astype(jnp.bfloat16)


def reference(x, src_len, expert_idx, ln_gain, ln_bias, w_query, b_query, w_key, w_value, b_value, w_attn_out, b_attn_out, w_fc1, b_fc1, w_fc2, b_fc2, w_router, w_exp_in, b_exp_in, w_exp_out, b_exp_out):
    positions = jnp.arange(SEQ_LEN)

    def row_layers(row_pair):
        row, length = row_pair
        key_ok = positions < length
        hidden = attention_row(row, key_ok, ln_gain[0], ln_bias[0], w_query[0], b_query[0], w_key[0], w_value[0], b_value[0], w_attn_out[0], b_attn_out[0])
        hidden = dense_ffn(hidden, ln_gain[1], ln_bias[1], w_fc1, b_fc1, w_fc2, b_fc2)
        hidden = attention_row(hidden, key_ok, ln_gain[2], ln_bias[2], w_query[1], b_query[1], w_key[1], w_value[1], b_value[1], w_attn_out[1], b_attn_out[1])
        normed = layer_norm(hidden, ln_gain[3], ln_bias[3])
        logits = jnp.dot(normed, w_router, preferred_element_type=jnp.float32)
        return hidden, normed.astype(jnp.bfloat16), logits

    residual, normed, logits = lax.map(row_layers, (x, src_len))
    grouped = (GROUPS, TOKENS_GROUP)
    valid = (positions[None, :] < src_len[:, None]).reshape(grouped)
    first = expert_idx[..., 0].reshape(grouped)
    second = expert_idx[..., 1].reshape(grouped)
    router_probs = jax.nn.softmax(logits, axis=-1).reshape(GROUPS, TOKENS_GROUP, EXPERTS)
    prob_first = jnp.take_along_axis(router_probs, first[..., None], axis=-1)[..., 0]
    prob_second = jnp.take_along_axis(router_probs, second[..., None], axis=-1)[..., 0]
    gate_first = prob_first / (prob_first + prob_second)
    gate_second = prob_second / (prob_first + prob_second)
    expert_ids = jnp.arange(EXPERTS)
    hot_first = ((first[..., None] == expert_ids) & valid[..., None]).astype(jnp.int32)
    hot_second = ((second[..., None] == expert_ids) & valid[..., None]).astype(jnp.int32)
    rank_first = jnp.cumsum(hot_first, axis=1) - 1
    rank_second = jnp.cumsum(hot_second, axis=1) - 1 + jnp.sum(hot_first, axis=1, keepdims=True)
    slot_first = jnp.sum(rank_first * hot_first, axis=-1)
    slot_second = jnp.sum(rank_second * hot_second, axis=-1)
    dest_first = jnp.where(valid & (slot_first < CAPACITY), first * CAPACITY + slot_first, DUMP_SLOT)
    dest_second = jnp.where(valid & (slot_second < CAPACITY), second * CAPACITY + slot_second, DUMP_SLOT)
    tables = jax.vmap(fill_table)(dest_first, dest_second)
    zero_row = jnp.zeros((GROUPS, 1, D_MODEL), jnp.bfloat16)
    padded = jnp.concatenate([normed.reshape(GROUPS, TOKENS_GROUP, D_MODEL), zero_row], axis=1)
    dispatched = jax.vmap(take_rows)(padded, tables)
    per_expert = dispatched.reshape(GROUPS, EXPERTS, CAPACITY, D_MODEL).transpose(1, 0, 2, 3).reshape(EXPERTS, GROUPS * CAPACITY, D_MODEL)
    expert_out = lax.map(run_expert, (per_expert, w_exp_in, b_exp_in, w_exp_out, b_exp_out))
    returned = expert_out.reshape(EXPERTS, GROUPS, CAPACITY, D_MODEL).transpose(1, 0, 2, 3).reshape(GROUPS, DUMP_SLOT, D_MODEL)
    returned = jnp.concatenate([returned, zero_row], axis=1)
    out_first = jax.vmap(take_rows)(returned, dest_first).astype(jnp.float32)
    out_second = jax.vmap(take_rows)(returned, dest_second).astype(jnp.float32)
    combined = gate_first[..., None] * out_first + gate_second[..., None] * out_second
    result = residual.reshape(GROUPS, TOKENS_GROUP, D_MODEL).astype(jnp.float32) + combined
    return result.astype(jnp.bfloat16).reshape(BATCH, SEQ_LEN, D_MODEL)
```

```python
import functools

import jax
import jax.numpy as jnp
from jax import lax
from jax.experimental import pallas as pl
from jax.experimental.pallas import tpu as pltpu
from jax.sharding import PartitionSpec as P

LN_EPS = 1e-5
MESH = pl.DeviceIdType.MESH
F32 = jnp.float32
BF16 = jnp.bfloat16
VMEM = pl.BlockSpec(memory_space=pltpu.VMEM)
SMEM = pl.BlockSpec(memory_space=pltpu.SMEM)


def dot_nn(a, b):
    return lax.dot_general(a, b, (((1,), (0,)), ((), ())), preferred_element_type=F32)


def dot_nt(a, b):
    return lax.dot_general(a, b, (((1,), (1,)), ((), ())), preferred_element_type=F32)


def layer_norm(block, gain, shift):
    block = block.astype(F32)
    centered = block - jnp.mean(block, axis=-1, keepdims=True)
    variance = jnp.mean(centered * centered, axis=-1, keepdims=True)
    return centered * lax.rsqrt(variance + LN_EPS) * gain + shift


def greet_partner():
    barrier = pltpu.get_barrier_semaphore()
    pl.semaphore_signal(barrier, inc=1, device_id={'tp': 1 - lax.axis_index('tp')}, device_id_type=MESH)


def await_partner():
    pl.semaphore_wait(pltpu.get_barrier_semaphore(), 1)


def to_partner(src, dst, send_sem, recv_sem):
    return pltpu.make_async_remote_copy(src_ref=src, dst_ref=dst, send_sem=send_sem, recv_sem=recv_sem, device_id={'tp': 1 - lax.axis_index('tp')}, device_id_type=MESH)


def attention_block(q_ref, kx_ref, vx_ref, ctx_ref, s_ref, p_ref, key_ok, row, block, chunk):
    for pair in range(q_ref.shape[1] // 128):
        lanes = slice(128 * pair, 128 * pair + 128)
        query = q_ref[pl.ds(row, block), lanes]
        for half in range(2):
            s_ref[half] = dot_nt(query, kx_ref[2 * pair + half])
        for half in range(2):
            for start in range(0, block, chunk):
                scores = jnp.where(key_ok, s_ref[half, start:start + chunk], -1e30)
                top = jnp.max(scores, axis=-1, keepdims=True)
                weights = jnp.exp(scores - top)
                scale = 1.0 / jnp.sum(weights, axis=-1, keepdims=True)
                p_ref[half, start:start + chunk] = (weights * scale).astype(BF16)
        context = dot_nn(p_ref[0], vx_ref[2 * pair]) + dot_nn(p_ref[1], vx_ref[2 * pair + 1])
        ctx_ref[:, lanes] = context.astype(BF16)


def attention_kernel(layer, norm, block, chunk, len_ref, x_ref, gain_ref, shift_ref, wq_ref, wk_ref, wv_ref, wo_ref, b_ref, bo_ref, out_ref, q_ref, kx_ref, vx_ref, ctx_ref, s_ref, p_ref, part_ref, recv_ref, send_sem, recv_sem):
    greet_partner()
    tokens = x_ref.shape[0]
    width = wq_ref.shape[1]
    steps = tokens // block
    gain, shift = gain_ref[norm:norm + 1], shift_ref[norm:norm + 1]
    bias_q, bias_v = b_ref[layer:layer + 1, :width], b_ref[layer:layer + 1, width:]
    lane = lax.broadcasted_iota(jnp.int32, (block, 128), 1)

    def project(step, carry):
        row = pl.multiple_of(step * block, block)
        normed = layer_norm(x_ref[pl.ds(row, block)], gain, shift).astype(BF16)
        query = (dot_nt(normed, wq_ref[layer]) + bias_q).astype(BF16)
        q_ref[pl.ds(row, block)] = (query.astype(F32) * 0.125).astype(BF16)
        keys = dot_nt(normed, wk_ref[layer])
        values = dot_nt(normed, wv_ref[layer]) + bias_v
        for head in range(width // 64):
            lanes = slice(128 * (head // 2), 128 * (head // 2) + 128)
            mine = (lane < 64) if head % 2 == 0 else (lane >= 64)
            kx_ref[head, pl.ds(row, block)] = jnp.where(mine, keys[:, lanes], 0.0).astype(BF16)
            vx_ref[head, pl.ds(row, block)] = jnp.where(mine, values[:, lanes], 0.0).astype(BF16)
        return carry

    lax.fori_loop(0, steps, project, 0)
    key_ok = lax.broadcasted_iota(jnp.int32, (chunk, tokens), 1) < len_ref[0]
    await_partner()

    def attend(step, carry):
        row = pl.multiple_of(step * block, block)
        attention_block(q_ref, kx_ref, vx_ref, ctx_ref, s_ref, p_ref, key_ok, row, block, chunk)
        part_ref[pl.ds(row, block)] = dot_nn(ctx_ref[...], wo_ref[layer]).astype(BF16)
        to_partner(part_ref.at[pl.ds(row, block)], recv_ref.at[pl.ds(row, block)], send_sem.at[step], recv_sem.at[step]).start()
        return carry

    lax.fori_loop(0, steps, attend, 0)

    def finish(step, carry):
        row = pl.multiple_of(step * block, block)
        to_partner(part_ref.at[pl.ds(row, block)], recv_ref.at[pl.ds(row, block)], send_sem.at[step], recv_sem.at[step]).wait()
        total = part_ref[pl.ds(row, block)].astype(F32) + recv_ref[pl.ds(row, block)].astype(F32)
        out_ref[pl.ds(row, block)] = (x_ref[pl.ds(row, block)].astype(F32) + total + bo_ref[layer:layer + 1]).astype(BF16)
        return carry

    lax.fori_loop(0, steps, finish, 0)


def attention_layer(layer, norm, collective_id, length, x, gain, shift, w_q, w_k, w_v, w_o, bias, b_o):
    tokens, d_model = x.shape
    width = w_q.shape[1]
    block, chunk = 256, 32
    steps = tokens // block
    return pl.pallas_call(
        functools.partial(attention_kernel, layer, norm, block, chunk),
        out_shape=jax.ShapeDtypeStruct((tokens, d_model), BF16),
        in_specs=[SMEM] + [VMEM] * 9,
        out_specs=VMEM,
        scratch_shapes=[
            pltpu.VMEM((tokens, width), BF16),
            pltpu.VMEM((width // 64, tokens, 128), BF16),
            pltpu.VMEM((width // 64, tokens, 128), BF16),
            pltpu.VMEM((block, width), BF16),
            pltpu.VMEM((2, block, tokens), F32),
            pltpu.VMEM((2, block, tokens), BF16),
            pltpu.VMEM((tokens, d_model), BF16),
            pltpu.VMEM((tokens, d_model), BF16),
            pltpu.SemaphoreType.DMA((steps,)),
            pltpu.SemaphoreType.DMA((steps,)),
        ],
        compiler_params=pltpu.CompilerParams(collective_id=collective_id, has_side_effects=True),
    )(length, x, gain, shift, w_q, w_k, w_v, w_o, bias, b_o)


def ffn_kernel(norm, block, x_ref, gain_ref, shift_ref, w1_ref, b1_ref, w2_ref, b2_ref, out_ref, part_ref, recv_ref, send_sem, recv_sem):
    greet_partner()
    steps = x_ref.shape[0] // block
    gain, shift = gain_ref[norm:norm + 1], shift_ref[norm:norm + 1]
    await_partner()

    def compute(step, carry):
        row = pl.multiple_of(step * block, block)
        normed = layer_norm(x_ref[pl.ds(row, block)], gain, shift).astype(BF16)
        inner = jnp.maximum(dot_nn(normed, w1_ref[...]) + b1_ref[...], 0.0).astype(BF16)
        part_ref[pl.ds(row, block)] = dot_nn(inner, w2_ref[...]).astype(BF16)
        to_partner(part_ref.at[pl.ds(row, block)], recv_ref.at[pl.ds(row, block)], send_sem.at[step], recv_sem.at[step]).start()
        return carry

    lax.fori_loop(0, steps, compute, 0)

    def finish(step, carry):
        row = pl.multiple_of(step * block, block)
        to_partner(part_ref.at[pl.ds(row, block)], recv_ref.at[pl.ds(row, block)], send_sem.at[step], recv_sem.at[step]).wait()
        total = part_ref[pl.ds(row, block)].astype(F32) + recv_ref[pl.ds(row, block)].astype(F32)
        out_ref[pl.ds(row, block)] = (x_ref[pl.ds(row, block)].astype(F32) + total + b2_ref[...]).astype(BF16)
        return carry

    lax.fori_loop(0, steps, finish, 0)


def dense_ffn(norm, collective_id, x, gain, shift, w1, b1, w2, b2):
    tokens, d_model = x.shape
    block = 256
    steps = tokens // block
    return pl.pallas_call(
        functools.partial(ffn_kernel, norm, block),
        out_shape=jax.ShapeDtypeStruct((tokens, d_model), BF16),
        in_specs=[VMEM] * 7,
        out_specs=VMEM,
        scratch_shapes=[
            pltpu.VMEM((tokens, d_model), BF16),
            pltpu.VMEM((tokens, d_model), BF16),
            pltpu.SemaphoreType.DMA((steps,)),
            pltpu.SemaphoreType.DMA((steps,)),
        ],
        compiler_params=pltpu.CompilerParams(collective_id=collective_id, has_side_effects=True),
    )(x, gain, shift, w1, b1, w2, b2)


def route_kernel(norm, capacity, len_ref, idx_ref, x_ref, gain_ref, shift_ref, wr_ref, disp_ref, meta_ref, normed_ref, logit_ref):
    tokens, d_model = x_ref.shape
    experts = wr_ref.shape[1]
    half = d_model // 2
    block = 256
    gain, shift = gain_ref[norm:norm + 1], shift_ref[norm:norm + 1]
    router = wr_ref[...].astype(BF16)
    for row in range(0, tokens, block):
        normed = layer_norm(x_ref[row:row + block], gain, shift).astype(BF16)
        normed_ref[row:row + block] = normed
        logit_ref[row:row + block] = dot_nn(normed, router)
    valid = lax.broadcasted_iota(jnp.int32, (1, tokens), 1) < len_ref[0]
    expert = lax.broadcasted_iota(jnp.int32, (experts, tokens), 0)
    first, second = idx_ref[0:1], idx_ref[1:2]
    hot_first = jnp.where((expert == first) & valid, 1.0, 0.0)
    hot_second = jnp.where((expert == second) & valid, 1.0, 0.0)
    earlier = (lax.broadcasted_iota(jnp.int32, (tokens, tokens), 0) < lax.broadcasted_iota(jnp.int32, (tokens, tokens), 1))
    earlier = jnp.where(earlier, 1.0, 0.0).astype(BF16)
    rank_first = dot_nn(hot_first.astype(BF16), earlier)
    rank_second = dot_nn(hot_second.astype(BF16), earlier) + jnp.sum(hot_first, axis=1, keepdims=True)
    slot_first = jnp.sum(rank_first * hot_first, axis=0, keepdims=True).astype(jnp.int32)
    slot_second = jnp.sum(rank_second * hot_second, axis=0, keepdims=True).astype(jnp.int32)
    dump = experts * capacity
    dest_first = jnp.where(valid & (slot_first < capacity), first * capacity + slot_first, dump)
    dest_second = jnp.where(valid & (slot_second < capacity), second * capacity + slot_second, dump)
    columns = pl.ds(pl.multiple_of(lax.axis_index('tp') * half, half), half)
    mine = normed_ref[:, columns]
    for slot in range(0, dump, block):
        slots = slot + lax.broadcasted_iota(jnp.int32, (block, tokens), 0)
        taken = jnp.where((slots == dest_first) | (slots == dest_second), 1.0, 0.0).astype(BF16)
        disp_ref[slot:slot + block] = dot_nn(taken, mine).astype(BF16)
    row_id = lax.broadcasted_iota(jnp.int32, (128, tokens), 0)
    packed = jnp.where(row_id == 0, dest_first, jnp.where(row_id == 1, dest_second, jnp.where(row_id == 2, first, second)))
    table = packed.astype(F32).T
    logits = logit_ref[...]
    lane = lax.broadcasted_iota(jnp.int32, (tokens, experts), 1).astype(F32)
    logit_first = jnp.sum(jnp.where(lane == table[:, 2:3], logits, 0.0), axis=1, keepdims=True)
    logit_second = jnp.sum(jnp.where(lane == table[:, 3:4], logits, 0.0), axis=1, keepdims=True)
    gate_first = jax.nn.sigmoid(logit_first - logit_second)
    gate_second = jax.nn.sigmoid(logit_second - logit_first)
    column = lax.broadcasted_iota(jnp.int32, (tokens, 128), 1)
    meta_ref[...] = jnp.where(column == 2, gate_first, jnp.where(column == 3, gate_second, table))


def route(norm, capacity, length, idx, x, gain, shift, w_router):
    tokens, d_model = x.shape
    experts = w_router.shape[1]
    return pl.pallas_call(
        functools.partial(route_kernel, norm, capacity),
        out_shape=(jax.ShapeDtypeStruct((experts * capacity, d_model // 2), BF16), jax.ShapeDtypeStruct((tokens, 128), F32)),
        in_specs=[SMEM] + [VMEM] * 5,
        out_specs=(VMEM, VMEM),
        scratch_shapes=[pltpu.VMEM((tokens, d_model), BF16), pltpu.VMEM((tokens, experts), F32)],
    )(length, idx, x, gain, shift, w_router)


def offset_peers(ep_size, me, step):
    if ep_size != 64:
        return lax.rem(me + step, ep_size), lax.rem(me + ep_size - step, ep_size)
    dy, dx = lax.rem(step // 4, 4), lax.rem(step, 4)
    dz = lax.rem(step // 16 + 8 - dy - dx, 4)
    z, y, x = me // 16, lax.rem(me // 4, 4), lax.rem(me, 4)
    ahead = lax.rem(z + dz, 4) * 16 + lax.rem(y + dy, 4) * 4 + lax.rem(x + dx, 4)
    behind = lax.rem(z + 4 - dz, 4) * 16 + lax.rem(y + 4 - dy, 4) * 4 + lax.rem(x + 4 - dx, 4)
    return ahead, behind


def experts_kernel(ep_size, groups, disp_ref, w1_ref, b1_ref, w2_ref, b2_ref, ret_ref, mine_ref, other_ref, keep_ref, give_ref, take_ref, out_ref, ship_send, ship_recv, swap_send, swap_recv, part_send, part_recv, ret_send, ret_recv):
    me, core = lax.axis_index('ep'), lax.axis_index('tp')
    local_experts, cap, half = disp_ref.shape[1:]
    each = ep_size // groups
    near = pl.ds(pl.multiple_of(core * half, half), half)
    far = pl.ds(pl.multiple_of((1 - core) * half, half), half)

    def slot_rows(step):
        return pl.ds(pl.multiple_of(lax.rem(step, each) * cap, cap), cap)

    def ship(step):
        ahead, _ = offset_peers(ep_size, me, step)
        return pltpu.make_async_remote_copy(src_ref=disp_ref.at[ahead], dst_ref=mine_ref.at[step // each, :, slot_rows(step)], send_sem=ship_send.at[step], recv_sem=ship_recv.at[step], device_id={'ep': ahead}, device_id_type=MESH)

    def ship_back(step):
        _, behind = offset_peers(ep_size, me, step)
        return pltpu.make_async_remote_copy(src_ref=out_ref.at[step // each, :, slot_rows(step)], dst_ref=ret_ref.at[me], send_sem=ret_send.at[step], recv_sem=ret_recv.at[step], device_id={'ep': behind}, device_id_type=MESH)

    def swap(group):
        return to_partner(mine_ref.at[group], other_ref.at[group], swap_send.at[group], swap_recv.at[group])

    def give(group):
        return to_partner(give_ref.at[group], take_ref.at[group], part_send.at[group], part_recv.at[group])

    barrier = pltpu.get_barrier_semaphore()

    def greet(step, carry):
        pl.semaphore_signal(barrier, inc=1, device_id={'ep': offset_peers(ep_size, me, step)[0]}, device_id_type=MESH)
        return carry

    lax.fori_loop(1, ep_size, greet, 0)
    greet_partner()
    mine_ref[0, :, 0:cap] = disp_ref[me]
    pl.semaphore_wait(barrier, ep_size)

    def send(step, carry):
        ship(step).start()
        return carry

    lax.fori_loop(1, ep_size, send, 0)

    def gather(group):
        def arrive(step, carry):
            ship(step).wait_recv()
            return carry

        lax.fori_loop(group * each + (1 if group == 0 else 0), (group + 1) * each, arrive, 0)
        swap(group).start()

    def compute(group):
        swap(group).wait_recv()
        for expert in range(local_experts):
            inner = dot_nn(mine_ref[group, expert], w1_ref[expert, near]) + dot_nn(other_ref[group, expert], w1_ref[expert, far])
            inner = jnp.maximum(inner + b1_ref[expert:expert + 1], 0.0).astype(BF16)
            give_ref[group, expert] = dot_nn(inner, w2_ref[expert, :, far]).astype(BF16)
            keep_ref[expert] = dot_nn(inner, w2_ref[expert, :, near]).astype(BF16)
        give(group).start()

    def deliver(group):
        give(group).wait_recv()
        for expert in range(local_experts):
            total = keep_ref[expert].astype(F32) + take_ref[group, expert].astype(F32)
            out_ref[group, expert] = (total + b2_ref[expert:expert + 1, near]).astype(BF16)

        def post(step, carry):
            ship_back(step).start()
            return carry

        lax.fori_loop(group * each + (1 if group == 0 else 0), (group + 1) * each, post, 0)

    for group in range(groups):
        gather(group)
        compute(group)
        deliver(group)
    ret_ref[me] = out_ref[0, :, 0:cap]

    def settle(step, carry):
        ship(step).wait_send()
        ship_back(step).wait()
        return carry

    lax.fori_loop(1, ep_size, settle, 0)
    for group in range(groups):
        swap(group).wait_send()
        give(group).wait_send()


def run_experts(ep_size, collective_id, dispatched, w1, b1, w2, b2):
    local_experts, d_model, width = w1.shape
    half = d_model // 2
    slots = dispatched.shape[0]
    cap = slots // (ep_size * local_experts)
    groups = 4 if ep_size >= 16 else 2
    rows = ep_size // groups * cap
    wide = pltpu.VMEM((groups, local_experts, rows, half), BF16)
    pair = pltpu.SemaphoreType.DMA((ep_size,))
    few = pltpu.SemaphoreType.DMA((groups,))
    return pl.pallas_call(
        functools.partial(experts_kernel, ep_size, groups),
        out_shape=jax.ShapeDtypeStruct((ep_size, local_experts, cap, half), BF16),
        in_specs=[VMEM] * 5,
        out_specs=VMEM,
        scratch_shapes=[wide, wide, pltpu.VMEM((local_experts, rows, half), BF16), wide, wide, wide, pair, pair, few, few, few, few, pair, pair],
        compiler_params=pltpu.CompilerParams(collective_id=collective_id, has_side_effects=True),
    )(dispatched.reshape(ep_size, local_experts, cap, half), w1, b1, w2, b2).reshape(slots, half)


def combine_kernel(block, x_ref, meta_ref, ret_ref, out_ref, mine_ref, other_ref, send_sem, recv_sem):
    greet_partner()
    core = lax.axis_index('tp')
    tokens, d_model = x_ref.shape
    slots, half = ret_ref.shape
    near = pl.ds(pl.multiple_of(core * half, half), half)
    far = pl.ds(pl.multiple_of((1 - core) * half, half), half)
    steps = tokens // block
    await_partner()
    slot = lax.broadcasted_iota(jnp.int32, (block, slots), 1)

    def pick(step, carry):
        rows = pl.ds(pl.multiple_of(step * block, block), block)
        meta = meta_ref[rows]
        dest = meta.astype(jnp.int32)
        first = dot_nn(jnp.where(slot == dest[:, 0:1], 1.0, 0.0).astype(BF16), ret_ref[...])
        second = dot_nn(jnp.where(slot == dest[:, 1:2], 1.0, 0.0).astype(BF16), ret_ref[...])
        result = (x_ref[rows, near].astype(F32) + (meta[:, 2:3] * first + meta[:, 3:4] * second)).astype(BF16)
        mine_ref[rows] = result
        to_partner(mine_ref.at[rows], other_ref.at[rows], send_sem.at[step], recv_sem.at[step]).start()
        out_ref[rows, near] = result
        return carry

    lax.fori_loop(0, steps, pick, 0)

    def finish(step, carry):
        rows = pl.ds(pl.multiple_of(step * block, block), block)
        to_partner(mine_ref.at[rows], other_ref.at[rows], send_sem.at[step], recv_sem.at[step]).wait()
        out_ref[rows, far] = other_ref[rows]
        return carry

    lax.fori_loop(0, steps, finish, 0)


def combine(collective_id, x, meta, returned):
    tokens, d_model = x.shape
    half = d_model // 2
    block = 256
    steps = tokens // block
    return pl.pallas_call(
        functools.partial(combine_kernel, block),
        out_shape=jax.ShapeDtypeStruct((tokens, d_model), BF16),
        in_specs=[VMEM] * 3,
        out_specs=VMEM,
        scratch_shapes=[pltpu.VMEM((tokens, half), BF16), pltpu.VMEM((tokens, half), BF16), pltpu.SemaphoreType.DMA((steps,)), pltpu.SemaphoreType.DMA((steps,))],
        compiler_params=pltpu.CompilerParams(collective_id=collective_id, has_side_effects=True),
    )(x, meta, returned)


def solution(mesh):
    ep_size = mesh.shape['ep']

    def local_fn(x, src_len, expert_idx, ln_gain, ln_bias, w_query, b_query, w_key, w_value, b_value, w_attn_out, b_attn_out, w_fc1, b_fc1, w_fc2, b_fc2, w_router, w_exp_in, b_exp_in, w_exp_out, b_exp_out):
        _, tokens, d_model = x.shape
        width = w_query.shape[2] * w_query.shape[3]
        num_experts = w_router.shape[1]
        capacity = 2 * (-(-tokens // num_experts))
        w_q, w_k, w_v = (jnp.transpose(w, (0, 2, 3, 1)).reshape(2, width, d_model) for w in (w_query, w_key, w_value))
        w_o = w_attn_out.reshape(2, width, d_model)
        bias = jnp.concatenate([b_query.reshape(2, width), b_value.reshape(2, width)], axis=1)
        idx = jnp.transpose(expert_idx, (0, 2, 1)).reshape(2, tokens)
        row = x.reshape(tokens, d_model)
        attention = functools.partial(attention_layer, gain=ln_gain, shift=ln_bias, w_q=w_q, w_k=w_k, w_v=w_v, w_o=w_o, bias=bias, b_o=b_attn_out)
        hidden = attention(0, 0, 1, src_len, row)
        hidden = dense_ffn(1, 2, hidden, ln_gain, ln_bias, w_fc1, b_fc1.reshape(1, -1), w_fc2, b_fc2.reshape(1, -1))
        hidden = attention(1, 2, 3, src_len, hidden)
        dispatched, meta = route(3, capacity, src_len, idx, hidden, ln_gain, ln_bias, w_router)
        returned = run_experts(ep_size, 4, dispatched, w_exp_in, b_exp_in, w_exp_out, b_exp_out)
        return combine(5, hidden, meta, returned).reshape(1, tokens, d_model)

    in_specs = (P(('dp', 'ep'), None, None), P(('dp', 'ep')), P(('dp', 'ep'), None, None), P(), P(), P(None, None, 'tp', None), P(None, 'tp', None), P(None, None, 'tp', None), P(None, None, 'tp', None), P(None, 'tp', None), P(None, 'tp', None, None), P(), P(None, 'tp'), P('tp'), P('tp', None), P(), P(), P('ep', None, 'tp'), P('ep', 'tp'), P('ep', 'tp', None), P('ep', None))
    return jax.shard_map(local_fn, mesh=mesh, in_specs=in_specs, out_specs=P(('dp', 'ep'), None, None), check_vma=False)
```

```python
import functools

import jax
import jax.numpy as jnp
from jax import lax
from jax.experimental import pallas as pl
from jax.experimental.pallas import tpu as pltpu
from jax.sharding import PartitionSpec as P

LN_EPS = 1e-5
MESH = pl.DeviceIdType.MESH
F32 = jnp.float32
BF16 = jnp.bfloat16
MIN_LEN = 256


def dot_nn(a, b):
    return lax.dot_general(a, b, (((1,), (0,)), ((), ())), preferred_element_type=F32)


def dot_nt(a, b):
    return lax.dot_general(a, b, (((1,), (1,)), ((), ())), preferred_element_type=F32)


def layer_norm(block, gain, shift):
    block = block.astype(F32)
    centered = block - jnp.mean(block, axis=-1, keepdims=True)
    variance = jnp.mean(centered * centered, axis=-1, keepdims=True)
    return centered * lax.rsqrt(variance + LN_EPS) * gain + shift


def iota(shape, axis):
    return lax.broadcasted_iota(jnp.int32, shape, axis)


def offset_peers(ep_size, me, step):
    if ep_size != 64:
        return lax.rem(me + step, ep_size), lax.rem(me + ep_size - step, ep_size)
    dy, dx = lax.rem(step // 4, 4), lax.rem(step, 4)
    dz = lax.rem(step // 16 + 8 - dy - dx, 4)
    z, y, x = me // 16, lax.rem(me // 4, 4), lax.rem(me, 4)
    ahead = lax.rem(z + dz, 4) * 16 + lax.rem(y + dy, 4) * 4 + lax.rem(x + dx, 4)
    behind = lax.rem(z + 4 - dz, 4) * 16 + lax.rem(y + 4 - dy, 4) * 4 + lax.rem(x + 4 - dx, 4)
    return ahead, behind


def offset_step(ep_size, me, device):
    if ep_size != 64:
        delta = device - me
        return jnp.where(delta < 0, delta + ep_size, delta)
    z, y, x = me // 16, lax.rem(me // 4, 4), lax.rem(me, 4)
    dz, dy, dx = ((device >> 4) - z) & 3, (((device >> 2) & 3) - y) & 3, ((device & 3) - x) & 3
    return (((dz + dy + dx) & 3) << 4) + (dy << 2) + dx


def encoder_kernel(ep_size, groups, block, chunk, len_ref, idx_ref, x_hbm, gain_ref, shift_ref, wq_hbm, wk_hbm, wv_hbm, wo_hbm, bq_ref, bv_ref, bo_ref, f1_hbm, fb1_ref, f2_hbm, fb2_ref, wr_hbm, e1_hbm, eb1_ref, e2_hbm, eb2_ref, out_ref,
                   hid_ref, wq_ref, wk_ref, wv_ref, wo_ref, f1_ref, f2_ref, wr_ref, e1_ref, e2_ref, load_sem, x_sem,
                   q_ref, kx_ref, vx_ref, ctx_ref, s_even, s_odd, p_even, p_odd, head_ref, part_ref, recv_ref, part_send, part_recv,
                   norm_ref, logit_ref, dest_ref, meta_ref, disp_ref, mine_ref, other_ref, keep_ref, give_ref, take_ref, done_ref, ret_ref,
                   ship_send, ship_recv, swap_send, swap_recv, give_send, give_recv, back_send, back_recv, acc_ref, near_ref, far_ref, half_send, half_recv):
    me, core = lax.axis_index('ep'), lax.axis_index('tp')
    tokens, d_model = hid_ref.shape
    steps = tokens // block
    width = q_ref.shape[1]
    local_experts, cap, half = disp_ref.shape[2:]
    experts = wr_ref.shape[1]
    each = ep_size // groups
    near = pl.ds(pl.multiple_of(core * half, half), half)
    far = pl.ds(pl.multiple_of((1 - core) * half, half), half)
    barrier = pltpu.get_barrier_semaphore()

    def rows_of(step):
        return pl.ds(pl.multiple_of(step * block, block), block)

    def to_partner(src, dst, send_sem, recv_sem):
        return pltpu.make_async_remote_copy(src_ref=src, dst_ref=dst, send_sem=send_sem, recv_sem=recv_sem, device_id={'tp': 1 - core}, device_id_type=MESH)

    def x_copy(step):
        return pltpu.make_async_copy(x_hbm.at[rows_of(step)], hid_ref.at[rows_of(step)], x_sem.at[step])

    pairs = [(wq_hbm, wq_ref), (wk_hbm, wk_ref), (wv_hbm, wv_ref), (wo_hbm, wo_ref), (f1_hbm, f1_ref), (f2_hbm, f2_ref), (wr_hbm, wr_ref), (e1_hbm, e1_ref), (e2_hbm, e2_ref)]
    loads = [pltpu.make_async_copy(src, dst, load_sem.at[index]) for index, (src, dst) in enumerate(pairs)]
    load_q, load_k, load_v, load_o, load_f1, load_f2, load_r, load_e1, load_e2 = loads

    def fetch_x(step, carry):
        x_copy(step).start()
        return carry

    lax.fori_loop(0, steps, fetch_x, 0)
    for load in loads:
        load.start()

    def greet(step, carry):
        pl.semaphore_signal(barrier, inc=1, device_id={'ep': offset_peers(ep_size, me, step)[0]}, device_id_type=MESH)
        return carry

    lax.fori_loop(1, ep_size, greet, 0)
    pl.semaphore_signal(barrier, inc=1, device_id={'tp': 1 - core}, device_id_type=MESH)

    def exchange(stage, step):
        return to_partner(part_ref.at[rows_of(step)], recv_ref.at[stage % 2, rows_of(step)], part_send.at[stage, step], part_recv.at[stage, step])

    def absorb(stage, step, bias):
        exchange(stage, step).wait()
        total = part_ref[rows_of(step)].astype(F32) + recv_ref[stage % 2, rows_of(step)].astype(F32)
        hidden = (hid_ref[rows_of(step)].astype(F32) + total + bias).astype(BF16)
        hid_ref[rows_of(step)] = hidden
        return hidden

    lane = iota((block, 128), 1)
    key_ok = iota((chunk, tokens - MIN_LEN), 1) + MIN_LEN < len_ref[0] if tokens > MIN_LEN else None

    def softmax(s_ref, p_ref):
        for start in range(0, block, chunk):
            scores = s_ref[start:start + chunk]
            if key_ok is not None:
                scores = jnp.concatenate([scores[:, :MIN_LEN], jnp.where(key_ok, scores[:, MIN_LEN:], -1e30)], axis=1)
            weights = jnp.exp(scores - jnp.max(scores, axis=-1, keepdims=True))
            scale = 1.0 / jnp.sum(weights, axis=-1, keepdims=True)
            p_ref[start:start + chunk] = (weights * scale).astype(BF16)

    def project(layer, step, normed):
        rows = rows_of(step)
        bias_q, bias_v = bq_ref[layer], bv_ref[layer]
        query = (dot_nt(normed, wq_ref[layer]) + bias_q).astype(BF16)
        q_ref[rows] = (query.astype(F32) * 0.125).astype(BF16)
        keys = dot_nt(normed, wk_ref[layer])
        values = dot_nt(normed, wv_ref[layer]) + bias_v
        for head in range(width // 64):
            lanes = slice(128 * (head // 2), 128 * (head // 2) + 128)
            mine = (lane < 64) if head % 2 == 0 else (lane >= 64)
            kx_ref[head, rows] = jnp.where(mine, keys[:, lanes], 0.0).astype(BF16)
            vx_ref[head, rows] = jnp.where(mine, values[:, lanes], 0.0).astype(BF16)

    def attend(layer, stage):
        heads = width // 64
        s_refs, p_refs = (s_even, s_odd), (p_even, p_odd)

        def score(rows, head):
            lanes = slice(128 * (head // 2), 128 * (head // 2) + 128)
            s_refs[head % 2][...] = dot_nt(q_ref[rows, lanes], kx_ref[head])

        def weigh(head):
            lanes = slice(128 * (head // 2), 128 * (head // 2) + 128)
            mixed = dot_nn(p_refs[head % 2][...], vx_ref[head])
            if head % 2 == 0:
                head_ref[...] = mixed
            else:
                ctx_ref[:, lanes] = (head_ref[...] + mixed).astype(BF16)

        def body(step, carry):
            rows = rows_of(step)
            score(rows, 0)
            for head in range(heads + 1):
                if head + 1 < heads:
                    score(rows, head + 1)
                if head > 0:
                    weigh(head - 1)
                if head < heads:
                    softmax(s_refs[head % 2], p_refs[head % 2])
            part_ref[rows] = dot_nn(ctx_ref[...], wo_ref[layer]).astype(BF16)
            exchange(stage, step).start()
            return carry

        lax.fori_loop(0, steps, body, 0)

    def normed_hidden(hidden, norm):
        return layer_norm(hidden, gain_ref[norm:norm + 1], shift_ref[norm:norm + 1]).astype(BF16)

    load_q.wait()
    load_k.wait()
    load_v.wait()

    def first_project(step, carry):
        x_copy(step).wait()
        project(0, step, normed_hidden(hid_ref[rows_of(step)], 0))
        return carry

    lax.fori_loop(0, steps, first_project, 0)
    load_o.wait()
    pl.semaphore_wait(barrier, ep_size)
    attend(0, 0)
    load_f1.wait()
    load_f2.wait()

    def feed(step, carry):
        normed = normed_hidden(absorb(0, step, bo_ref[0:1]), 1)
        inner = jnp.maximum(dot_nn(normed, f1_ref[...]) + fb1_ref[...], 0.0).astype(BF16)
        part_ref[rows_of(step)] = dot_nn(inner, f2_ref[...]).astype(BF16)
        exchange(1, step).start()
        return carry

    lax.fori_loop(0, steps, feed, 0)

    def second_project(step, carry):
        project(1, step, normed_hidden(absorb(1, step, fb2_ref[...]), 2))
        return carry

    lax.fori_loop(0, steps, second_project, 0)
    attend(1, 2)

    valid = iota((1, tokens), 1) < len_ref[0]
    first, second = idx_ref[0:1], idx_ref[1:2]
    expert = iota((experts, tokens), 0)
    hot_first = jnp.where((expert == first) & valid, 1.0, 0.0)
    hot_second = jnp.where((expert == second) & valid, 1.0, 0.0)
    earlier = jnp.where(iota((tokens, tokens), 0) < iota((tokens, tokens), 1), 1.0, 0.0).astype(BF16)
    rank_first = dot_nn(hot_first.astype(BF16), earlier)
    rank_second = dot_nn(hot_second.astype(BF16), earlier) + jnp.sum(hot_first, axis=1, keepdims=True)
    slot_first = jnp.sum(rank_first * hot_first, axis=0, keepdims=True).astype(jnp.int32)
    slot_second = jnp.sum(rank_second * hot_second, axis=0, keepdims=True).astype(jnp.int32)

    def place(choice, slot):
        step = offset_step(ep_size, me, choice >> 1)
        return jnp.where(valid & (slot < cap), ((step << 1) + (choice & 1)) * cap + slot, experts * cap)

    dest_ref[0:1] = place(first, slot_first)
    dest_ref[1:2] = place(second, slot_second)
    load_r.wait()
    router = wr_ref[...].astype(BF16)

    def settle(step, carry):
        normed = normed_hidden(absorb(2, step, bo_ref[1:2]), 3)
        norm_ref[rows_of(step)] = normed
        logit_ref[rows_of(step)] = dot_nn(normed, router)
        return carry

    lax.fori_loop(0, steps, settle, 0)

    def slot_rows(step):
        return pl.ds(pl.multiple_of(lax.rem(step, each) * cap, cap), cap)

    def ship(step):
        ahead, _ = offset_peers(ep_size, me, step)
        return pltpu.make_async_remote_copy(src_ref=disp_ref.at[step // each, lax.rem(step, each)], dst_ref=mine_ref.at[step // each, :, slot_rows(step)], send_sem=ship_send.at[step], recv_sem=ship_recv.at[step], device_id={'ep': ahead}, device_id_type=MESH)

    def ship_back(step):
        _, behind = offset_peers(ep_size, me, step)
        return pltpu.make_async_remote_copy(src_ref=done_ref.at[step // each, :, slot_rows(step)], dst_ref=ret_ref.at[step // each, lax.rem(step, each)], send_sem=back_send.at[step], recv_sem=back_recv.at[step], device_id={'ep': behind}, device_id_type=MESH)

    def swap(group):
        return to_partner(mine_ref.at[group], other_ref.at[group], swap_send.at[group], swap_recv.at[group])

    def give(group):
        return to_partner(give_ref.at[group], take_ref.at[group], give_send.at[group], give_recv.at[group])

    def each_step(group, act):
        def body(step, carry):
            act(step)
            return carry

        lax.fori_loop(jnp.where(group == 0, 1, group * each), (group + 1) * each, body, 0)

    members = each * local_experts * cap

    def scatter(group, carry):
        slots = iota((members, tokens), 0) + group * members
        taken = jnp.where((slots == dest_ref[0:1]) | (slots == dest_ref[1:2]), 1.0, 0.0).astype(BF16)
        disp_ref[group] = dot_nn(taken, norm_ref[:, near]).astype(BF16).reshape(each, local_experts, cap, half)
        each_step(group, lambda step: ship(step).start())
        return carry

    lax.fori_loop(0, groups, scatter, 0)
    mine_ref[0, :, 0:cap] = disp_ref[0, 0]

    row_id = iota((128, tokens), 0)
    packed = jnp.where(row_id == 0, dest_ref[0:1], jnp.where(row_id == 1, dest_ref[1:2], jnp.where(row_id == 2, first, second)))
    meta_ref[...] = packed.astype(F32).T
    column = iota((block, experts), 1).astype(F32)
    spot = iota((block, 128), 1)

    def gate(step, carry):
        table, logits = meta_ref[rows_of(step)], logit_ref[rows_of(step)]
        logit_first = jnp.sum(jnp.where(column == table[:, 2:3], logits, 0.0), axis=1, keepdims=True)
        logit_second = jnp.sum(jnp.where(column == table[:, 3:4], logits, 0.0), axis=1, keepdims=True)
        gate_first = jax.nn.sigmoid(logit_first - logit_second)
        gate_second = jax.nn.sigmoid(logit_second - logit_first)
        meta_ref[rows_of(step)] = jnp.where(spot == 2, gate_first, jnp.where(spot == 3, gate_second, table))
        acc_ref[rows_of(step)] = hid_ref[rows_of(step), near].astype(F32)
        return carry

    lax.fori_loop(0, steps, gate, 0)
    load_e1.wait()
    load_e2.wait()

    def deliver(group):
        give(group).wait_recv()
        for expert in range(local_experts):
            total = keep_ref[expert].astype(F32) + take_ref[group, expert].astype(F32)
            done_ref[group, expert] = (total + eb2_ref[expert:expert + 1, near]).astype(BF16)
        each_step(group, lambda step: ship_back(step).start())

    def work(group, carry):
        each_step(group, lambda step: ship(step).wait_recv())
        swap(group).start()

        @pl.when(group > 0)
        def _():
            deliver(group - 1)

        swap(group).wait_recv()
        for expert in range(local_experts):
            inner = dot_nn(mine_ref[group, expert], e1_ref[expert, near]) + dot_nn(other_ref[group, expert], e1_ref[expert, far])
            inner = jnp.maximum(inner + eb1_ref[expert:expert + 1], 0.0).astype(BF16)
            give_ref[group, expert] = dot_nn(inner, e2_ref[expert, :, far]).astype(BF16)
            keep_ref[expert] = dot_nn(inner, e2_ref[expert, :, near]).astype(BF16)
        give(group).start()
        return carry

    lax.fori_loop(0, groups, work, 0)
    deliver(groups - 1)
    ret_ref[0, 0] = done_ref[0, :, 0:cap]

    def halves(step):
        return to_partner(near_ref.at[rows_of(step)], far_ref.at[rows_of(step)], half_send.at[step], half_recv.at[step])

    def gather(group, carry):
        each_step(group, lambda step: ship_back(step).wait_recv())
        slots = iota((block, members), 1) + group * members

        def pick(step, carry):
            rows = rows_of(step)
            table = meta_ref[rows]
            dest = table.astype(jnp.int32)
            returned = ret_ref[group].reshape(members, half)
            one = dot_nn(jnp.where(slots == dest[:, 0:1], 1.0, 0.0).astype(BF16), returned)
            two = dot_nn(jnp.where(slots == dest[:, 1:2], 1.0, 0.0).astype(BF16), returned)
            result = acc_ref[rows] + (table[:, 2:3] * one + table[:, 3:4] * two)
            acc_ref[rows] = result

            @pl.when(group == groups - 1)
            def _():
                near_ref[rows] = result.astype(BF16)
                halves(step).start()
                out_ref[rows, near] = result.astype(BF16)

            return carry

        lax.fori_loop(0, steps, pick, 0)
        return carry

    lax.fori_loop(0, groups, gather, 0)

    def finish(step, carry):
        halves(step).wait()
        out_ref[rows_of(step), far] = far_ref[rows_of(step)]
        return carry

    lax.fori_loop(0, steps, finish, 0)

    def drain(step, carry):
        ship(step).wait_send()
        ship_back(step).wait_send()
        return carry

    lax.fori_loop(1, ep_size, drain, 0)

    def drain_pairs(group, carry):
        swap(group).wait_send()
        give(group).wait_send()
        return carry

    lax.fori_loop(0, groups, drain_pairs, 0)


def solution(mesh):
    ep_size = mesh.shape['ep']

    def local_fn(x, src_len, expert_idx, ln_gain, ln_bias, w_query, b_query, w_key, w_value, b_value, w_attn_out, b_attn_out, w_fc1, b_fc1, w_fc2, b_fc2, w_router, w_exp_in, b_exp_in, w_exp_out, b_exp_out):
        _, tokens, d_model = x.shape
        width = w_query.shape[2] * w_query.shape[3]
        num_experts = w_router.shape[1]
        local_experts, _, hidden = w_exp_in.shape
        cap = 2 * (-(-tokens // num_experts))
        half = d_model // 2
        groups = 4 if ep_size >= 16 else 2
        each = ep_size // groups
        block, chunk = min(256, tokens // 2), 32
        steps = tokens // block
        w_q, w_k, w_v = (jnp.transpose(w, (0, 2, 3, 1)).reshape(2, width, d_model) for w in (w_query, w_key, w_value))
        w_o = w_attn_out.reshape(2, width, d_model)
        idx = jnp.transpose(expert_idx, (0, 2, 1)).reshape(2, tokens)
        vmem = lambda *shape: pltpu.VMEM(shape, BF16)
        vmem32 = lambda *shape: pltpu.VMEM(shape, F32)
        dma = lambda *shape: pltpu.SemaphoreType.DMA(shape)
        whole = pl.BlockSpec(memory_space=pltpu.VMEM)
        far_away = pl.BlockSpec(memory_space=pl.ANY)
        rows = each * cap
        wide = vmem(groups, local_experts, rows, half)
        blocks = vmem(groups, each, local_experts, cap, half)
        result = pl.pallas_call(
            functools.partial(encoder_kernel, ep_size, groups, block, chunk),
            out_shape=jax.ShapeDtypeStruct((tokens, d_model), BF16),
            in_specs=[pl.BlockSpec(memory_space=pltpu.SMEM), whole, far_away, whole, whole, far_away, far_away, far_away, far_away, whole, whole, whole, far_away, whole, far_away, whole, far_away, far_away, whole, far_away, whole],
            out_specs=whole,
            scratch_shapes=[
                vmem(tokens, d_model), vmem(2, width, d_model), vmem(2, width, d_model), vmem(2, width, d_model), vmem(2, width, d_model), vmem(*w_fc1.shape), vmem(*w_fc2.shape), vmem32(*w_router.shape), vmem(*w_exp_in.shape), vmem(*w_exp_out.shape), dma(9), dma(steps),
                vmem(tokens, width), vmem(width // 64, tokens, 128), vmem(width // 64, tokens, 128), vmem(block, width), vmem32(block, tokens), vmem32(block, tokens), vmem(block, tokens), vmem(block, tokens), vmem32(block, 128), vmem(tokens, d_model), vmem(2, tokens, d_model), dma(3, steps), dma(3, steps),
                vmem(tokens, d_model), vmem32(tokens, num_experts), pltpu.VMEM((8, tokens), jnp.int32), vmem32(tokens, 128), blocks, wide, wide, vmem(local_experts, rows, half), wide, wide, wide, blocks,
                dma(ep_size), dma(ep_size), dma(groups), dma(groups), dma(groups), dma(groups), dma(ep_size), dma(ep_size), vmem32(tokens, half), vmem(tokens, half), vmem(tokens, half), dma(steps), dma(steps),
            ],
            compiler_params=pltpu.CompilerParams(collective_id=1, has_side_effects=True, vmem_limit_bytes=67043328),
        )(src_len, idx, x.reshape(tokens, d_model), ln_gain, ln_bias, w_q, w_k, w_v, w_o, b_query.reshape(2, 1, width), b_value.reshape(2, 1, width), b_attn_out, w_fc1, b_fc1.reshape(1, -1), w_fc2, b_fc2.reshape(1, -1), w_router, w_exp_in, b_exp_in, w_exp_out, b_exp_out)
        return result.reshape(1, tokens, d_model)

    in_specs = (P(('dp', 'ep'), None, None), P(('dp', 'ep')), P(('dp', 'ep'), None, None), P(), P(), P(None, None, 'tp', None), P(None, 'tp', None), P(None, None, 'tp', None), P(None, None, 'tp', None), P(None, 'tp', None), P(None, 'tp', None, None), P(), P(None, 'tp'), P('tp'), P('tp', None), P(), P(), P('ep', None, 'tp'), P('ep', 'tp'), P('ep', 'tp', None), P('ep', None))
    return jax.shard_map(local_fn, mesh=mesh, in_specs=in_specs, out_specs=P(('dp', 'ep'), None, None), check_vma=False)
```

```python
import functools

import jax
import jax.numpy as jnp
from jax import lax
from jax.experimental import pallas as pl
from jax.experimental.pallas import tpu as pltpu
from jax.sharding import PartitionSpec as P

LN_EPS = 1e-5
MESH = pl.DeviceIdType.MESH
F32 = jnp.float32
BF16 = jnp.bfloat16
MIN_LEN = 256


def dot_nn(a, b):
    return lax.dot_general(a, b, (((1,), (0,)), ((), ())), preferred_element_type=F32)


def dot_nt(a, b):
    return lax.dot_general(a, b, (((1,), (1,)), ((), ())), preferred_element_type=F32)


def layer_norm(block, gain, shift):
    block = block.astype(F32)
    centered = block - jnp.mean(block, axis=-1, keepdims=True)
    variance = jnp.mean(centered * centered, axis=-1, keepdims=True)
    return centered * lax.rsqrt(variance + LN_EPS) * gain + shift


def iota(shape, axis):
    return lax.broadcasted_iota(jnp.int32, shape, axis)


def send_order(ep_size):
    if ep_size != 64:
        return [(step,) for step in range(1, ep_size)] + [(0,)]

    def at(axis, value, rest):
        return tuple(rest[:axis]) + (value,) + tuple(rest[axis:])

    def both(offset):
        return [offset, tuple(-v % 4 for v in offset)]

    order = [o for signs in ((1, 1, 1), (1, 1, 3), (1, 3, 1), (3, 1, 1)) for o in both(signs)]
    for axis in range(3):
        for rest in ((1, 1), (1, 3)):
            order += both(at(axis, 2, rest)) + both(at(axis, 0, rest))
    for axis in range(3):
        order += both(at(axis, 1, (2, 2))) + both(at(axis, 1, (0, 0)))
    for axis in range(3):
        order += [at(axis, 2, (0, 0)), at(axis, 0, (2, 2))]
    order += [(2, 2, 2)]
    order += both((2, 1, 0)) + both((0, 2, 1)) + both((1, 0, 2)) + both((2, 0, 1)) + both((1, 2, 0)) + both((0, 1, 2))
    return order + [(0, 0, 0)]


def peer(ep_size, me, offset, sign):
    if ep_size != 64:
        return lax.rem(me + ep_size + sign * offset[0], ep_size)
    z, y, x = me // 16, lax.rem(me // 4, 4), lax.rem(me, 4)
    dz, dy, dx = ((sign * v) % 4 for v in offset)
    return lax.rem(z + dz, 4) * 16 + lax.rem(y + dy, 4) * 4 + lax.rem(x + dx, 4)


def order_place(ep_size, me, device):
    order = send_order(ep_size)
    if ep_size != 64:
        delta = device - me
        delta = jnp.where(delta < 0, delta + ep_size, delta)
        codes = [offset[0] for offset in order]
    else:
        z, y, x = me // 16, lax.rem(me // 4, 4), lax.rem(me, 4)
        delta = ((((device >> 4) - z) & 3) << 4) + (((((device >> 2) & 3) - y) & 3) << 2) + (((device & 3) - x) & 3)
        codes = [16 * dz + 4 * dy + dx for dz, dy, dx in order]
    place = jnp.zeros_like(device)
    for index, code in enumerate(codes):
        place = jnp.where(delta == code, index, place)
    return place


def encoder_kernel(ep_size, groups, block, chunk, len_ref, idx_hbm, x_hbm, gain_hbm, shift_hbm, wq_hbm, wk_hbm, wv_hbm, wo_hbm, bq_hbm, bv_hbm, bo_hbm, f1_hbm, fb1_hbm, f2_hbm, fb2_hbm, wr_hbm, e1_hbm, eb1_hbm, e2_hbm, eb2_hbm, out_hbm,
                   hid_ref, wq_ref, wk_ref, wv_ref, wo_ref, f1_ref, f2_ref, wr_ref, e1_ref, e2_ref, idx_ref, gain_ref, shift_ref, bq_ref, bv_ref, bo_ref, fb1_ref, fb2_ref, eb1_ref, eb2_ref, load_sem, x_sem,
                   q_ref, kx_ref, vx_ref, ctx_ref, s_even, s_odd, p_even, p_odd, head_ref, part_ref, recv_ref, part_send, part_recv,
                   norm_ref, logit_ref, dest_ref, meta_ref, disp_ref, mine_ref, other_ref, keep_ref, give_ref, take_ref, done_ref, ret_ref,
                   ship_send, ship_recv, swap_send, swap_recv, give_send, give_recv, back_send, back_recv, acc_ref, near_ref, keep_sem, half_send, half_recv):
    me, core = lax.axis_index('ep'), lax.axis_index('tp')
    tokens, d_model = hid_ref.shape
    steps = tokens // block
    width = q_ref.shape[1]
    local_experts, cap, half = disp_ref.shape[2:]
    experts = wr_ref.shape[1]
    each = ep_size // groups
    near = pl.ds(pl.multiple_of(core * half, half), half)
    far = pl.ds(pl.multiple_of((1 - core) * half, half), half)
    barrier = pltpu.get_barrier_semaphore()

    def rows_of(step):
        return pl.ds(pl.multiple_of(step * block, block), block)

    def to_partner(src, dst, send_sem, recv_sem):
        return pltpu.make_async_remote_copy(src_ref=src, dst_ref=dst, send_sem=send_sem, recv_sem=recv_sem, device_id={'tp': 1 - core}, device_id_type=MESH)

    def x_copy(step):
        return pltpu.make_async_copy(x_hbm.at[rows_of(step)], hid_ref.at[rows_of(step)], x_sem.at[step])

    loads = {}

    def load(name, src, dst):
        loads[name] = pltpu.make_async_copy(src, dst, load_sem.at[len(loads)])
        loads[name].start()

    def loaded(*names):
        for name in names:
            loads[name].wait()

    for step in range(steps):
        x_copy(step).start()
    load('gain', gain_hbm, gain_ref)
    load('shift', shift_hbm, shift_ref)
    load('q0', wq_hbm.at[0], wq_ref.at[0])
    load('k0', wk_hbm.at[0], wk_ref.at[0])
    load('v0', wv_hbm.at[0], wv_ref.at[0])
    load('bq', bq_hbm, bq_ref)
    load('bv', bv_hbm, bv_ref)
    order = send_order(ep_size)
    last = ep_size - 1
    for offset in order[:last]:
        pl.semaphore_signal(barrier, inc=1, device_id={'ep': peer(ep_size, me, offset, 1)}, device_id_type=MESH)
    pl.semaphore_signal(barrier, inc=1, device_id={'tp': 1 - core}, device_id_type=MESH)

    def exchange(stage, step):
        return to_partner(part_ref.at[rows_of(step)], recv_ref.at[stage % 2, rows_of(step)], part_send.at[stage, step], part_recv.at[stage, step])

    def two_by_two(await_step, act):
        def body(pair, carry):
            for step in (2 * pair, 2 * pair + 1):
                await_step(step)
            for step in (2 * pair, 2 * pair + 1):
                act(step)
            return carry

        lax.fori_loop(0, steps // 2, body, 0)

    def absorb(stage, step, bias):
        total = part_ref[rows_of(step)].astype(F32) + recv_ref[stage % 2, rows_of(step)].astype(F32)
        hidden = (hid_ref[rows_of(step)].astype(F32) + total + bias).astype(BF16)
        hid_ref[rows_of(step)] = hidden
        return hidden

    lane = iota((block, 128), 1)
    key_ok = iota((chunk, tokens - MIN_LEN), 1) + MIN_LEN < len_ref[0] if tokens > MIN_LEN else None

    def softmax(s_ref, p_ref):
        for start in range(0, block, chunk):
            scores = s_ref[start:start + chunk]
            if key_ok is not None:
                scores = jnp.concatenate([scores[:, :MIN_LEN], jnp.where(key_ok, scores[:, MIN_LEN:], -1e30)], axis=1)
            weights = jnp.exp(scores - jnp.max(scores, axis=-1, keepdims=True))
            scale = 1.0 / jnp.sum(weights, axis=-1, keepdims=True)
            p_ref[start:start + chunk] = (weights * scale).astype(BF16)

    def project(layer, step, normed):
        rows = rows_of(step)
        bias_q, bias_v = (jnp.concatenate([ref[head, layer:layer + 1] for head in range(width // 64)], axis=1) for ref in (bq_ref, bv_ref))
        query = (dot_nt(normed, wq_ref[layer]) + bias_q).astype(BF16)
        q_ref[rows] = (query.astype(F32) * 0.125).astype(BF16)
        keys = dot_nt(normed, wk_ref[layer])
        values = dot_nt(normed, wv_ref[layer]) + bias_v
        for head in range(width // 64):
            lanes = slice(128 * (head // 2), 128 * (head // 2) + 128)
            mine = (lane < 64) if head % 2 == 0 else (lane >= 64)
            kx_ref[head, rows] = jnp.where(mine, keys[:, lanes], 0.0).astype(BF16)
            vx_ref[head, rows] = jnp.where(mine, values[:, lanes], 0.0).astype(BF16)

    def attend(layer, stage):
        heads = width // 64
        s_refs, p_refs = (s_even, s_odd), (p_even, p_odd)

        def score(rows, head):
            lanes = slice(128 * (head // 2), 128 * (head // 2) + 128)
            s_refs[head % 2][...] = dot_nt(q_ref[rows, lanes], kx_ref[head])

        def weigh(head):
            lanes = slice(128 * (head // 2), 128 * (head // 2) + 128)
            mixed = dot_nn(p_refs[head % 2][...], vx_ref[head])
            if head % 2 == 0:
                head_ref[...] = mixed
            else:
                ctx_ref[:, lanes] = (head_ref[...] + mixed).astype(BF16)

        def body(step, carry):
            rows = rows_of(step)
            score(rows, 0)
            for head in range(heads + 1):
                if head + 1 < heads:
                    score(rows, head + 1)
                if head > 0:
                    weigh(head - 1)
                if head < heads:
                    softmax(s_refs[head % 2], p_refs[head % 2])
            part_ref[rows] = dot_nn(ctx_ref[...], wo_ref[layer]).astype(BF16)
            exchange(stage, step).start()
            return carry

        lax.fori_loop(0, steps, body, 0, unroll=2)

    def normed_hidden(hidden, norm):
        return layer_norm(hidden, gain_ref[norm:norm + 1], shift_ref[norm:norm + 1]).astype(BF16)

    loaded('gain', 'shift', 'bq', 'bv', 'q0', 'k0', 'v0')
    load('o', wo_hbm, wo_ref)
    load('bo', bo_hbm, bo_ref)
    load('f1', f1_hbm, f1_ref)
    load('fb1', fb1_hbm, fb1_ref)
    load('f2', f2_hbm, f2_ref)
    load('fb2', fb2_hbm, fb2_ref)
    for step in range(steps):
        x_copy(step).wait()
    for step in range(steps):
        project(0, step, normed_hidden(hid_ref[rows_of(step)], 0))
    loaded('o', 'bo', 'f1', 'fb1', 'f2', 'fb2')
    load('q1', wq_hbm.at[1], wq_ref.at[1])
    load('k1', wk_hbm.at[1], wk_ref.at[1])
    load('v1', wv_hbm.at[1], wv_ref.at[1])
    load('idx', idx_hbm, idx_ref)
    load('r', wr_hbm, wr_ref)
    load('e1', e1_hbm, e1_ref)
    load('eb1', eb1_hbm, eb1_ref)
    load('e2', e2_hbm, e2_ref)
    load('eb2', eb2_hbm, eb2_ref)
    pl.semaphore_wait(barrier, ep_size)
    attend(0, 0)

    def feed(step):
        normed = normed_hidden(absorb(0, step, bo_ref[0:1]), 1)
        inner = jnp.maximum(dot_nn(normed, f1_ref[...]) + fb1_ref[...].reshape(1, -1), 0.0).astype(BF16)
        part_ref[rows_of(step)] = dot_nn(inner, f2_ref[...]).astype(BF16)
        exchange(1, step).start()

    two_by_two(lambda step: exchange(0, step).wait(), feed)
    loaded('q1', 'k1', 'v1')

    def second_project(step):
        project(1, step, normed_hidden(absorb(1, step, fb2_ref[...].reshape(1, -1)), 2))

    two_by_two(lambda step: exchange(1, step).wait(), second_project)
    attend(1, 2)
    loaded('idx', 'r')

    valid = iota((1, tokens), 1) < len_ref[0]
    first, second = idx_ref[0:1], idx_ref[1:2]
    expert = iota((experts, tokens), 0)
    hot_first = jnp.where((expert == first) & valid, 1.0, 0.0)
    hot_second = jnp.where((expert == second) & valid, 1.0, 0.0)
    earlier = jnp.where(iota((tokens, tokens), 0) < iota((tokens, tokens), 1), 1.0, 0.0).astype(BF16)
    rank_first = dot_nn(hot_first.astype(BF16), earlier)
    rank_second = dot_nn(hot_second.astype(BF16), earlier) + jnp.sum(hot_first, axis=1, keepdims=True)
    slot_first = jnp.sum(rank_first * hot_first, axis=0, keepdims=True).astype(jnp.int32)
    slot_second = jnp.sum(rank_second * hot_second, axis=0, keepdims=True).astype(jnp.int32)

    choice, slot = idx_ref[...], jnp.concatenate([slot_first, slot_second], axis=0)
    home = ((order_place(ep_size, me, choice >> 1) << 1) + (choice & 1)) * cap + slot
    dest_ref[0:2] = jnp.where(valid & (slot < cap), home, experts * cap)
    router = wr_ref[...].astype(BF16)

    def settle(step):
        normed = normed_hidden(absorb(2, step, bo_ref[1:2]), 3)
        norm_ref[rows_of(step)] = normed
        logit_ref[rows_of(step)] = dot_nn(normed, router)

    two_by_two(lambda step: exchange(2, step).wait(), settle)

    def slot_rows(step):
        return pl.ds(step % each * cap, cap)

    def ship(step):
        return pltpu.make_async_remote_copy(src_ref=disp_ref.at[step // each, step % each], dst_ref=mine_ref.at[step // each, :, slot_rows(step)], send_sem=ship_send.at[step], recv_sem=ship_recv.at[step], device_id={'ep': peer(ep_size, me, order[step], 1)}, device_id_type=MESH)

    def ship_back(step):
        return pltpu.make_async_remote_copy(src_ref=done_ref.at[step // each, :, slot_rows(step)], dst_ref=ret_ref.at[step // each, step % each], send_sem=back_send.at[step], recv_sem=back_recv.at[step], device_id={'ep': peer(ep_size, me, order[step], -1)}, device_id_type=MESH)

    def swap(group):
        return to_partner(mine_ref.at[group], other_ref.at[group], swap_send.at[group], swap_recv.at[group])

    def give(group):
        return to_partner(give_ref.at[group], take_ref.at[group], give_send.at[group], give_recv.at[group])

    def each_step(group, act):
        for index in range(groups):
            @pl.when(group == index)
            def _(index=index):
                for step in range(index * each, min((index + 1) * each, last)):
                    act(step)

    members = each * local_experts * cap

    def scatter(group, carry):
        slots = iota((members, tokens), 0) + group * members
        taken = jnp.where((slots == dest_ref[0:1]) | (slots == dest_ref[1:2]), 1.0, 0.0).astype(BF16)
        disp_ref[group] = dot_nn(taken, norm_ref[:, near]).astype(BF16).reshape(each, local_experts, cap, half)
        each_step(group, lambda step: ship(step).start())
        return carry

    lax.fori_loop(0, groups, scatter, 0)
    mine_ref[groups - 1, :, slot_rows(last)] = disp_ref[groups - 1, each - 1]

    row_id = iota((128, tokens), 0)
    packed = jnp.where(row_id == 0, dest_ref[0:1], jnp.where(row_id == 1, dest_ref[1:2], jnp.where(row_id == 2, first, second)))
    meta_ref[...] = packed.astype(F32).T
    column = iota((block, experts), 1).astype(F32)
    spot = iota((block, 128), 1)

    def gate(step, carry):
        table, logits = meta_ref[rows_of(step)], logit_ref[rows_of(step)]
        logit_first = jnp.sum(jnp.where(column == table[:, 2:3], logits, 0.0), axis=1, keepdims=True)
        logit_second = jnp.sum(jnp.where(column == table[:, 3:4], logits, 0.0), axis=1, keepdims=True)
        gate_first = jax.nn.sigmoid(logit_first - logit_second)
        gate_second = jax.nn.sigmoid(logit_second - logit_first)
        meta_ref[rows_of(step)] = jnp.where(spot == 2, gate_first, jnp.where(spot == 3, gate_second, table))
        acc_ref[rows_of(step)] = hid_ref[rows_of(step), near].astype(F32)
        return carry

    lax.fori_loop(0, steps, gate, 0)
    loaded('e1', 'eb1', 'e2', 'eb2')

    def deliver(group):
        give(group).wait_recv()
        for expert in range(local_experts):
            total = keep_ref[expert].astype(F32) + take_ref[group, expert].astype(F32)
            done_ref[group, expert] = (total + eb2_ref[expert:expert + 1, near]).astype(BF16)
        each_step(group, lambda step: ship_back(step).start())

    def work(group, carry):
        each_step(group, lambda step: ship(step).wait_recv())
        swap(group).start()

        @pl.when(group > 0)
        def _():
            deliver(group - 1)

        swap(group).wait_recv()
        for expert in range(local_experts):
            inner = dot_nn(mine_ref[group, expert], e1_ref[expert, near]) + dot_nn(other_ref[group, expert], e1_ref[expert, far])
            inner = jnp.maximum(inner + eb1_ref[expert:expert + 1], 0.0).astype(BF16)
            give_ref[group, expert] = dot_nn(inner, e2_ref[expert, :, far]).astype(BF16)
            keep_ref[expert] = dot_nn(inner, e2_ref[expert, :, near]).astype(BF16)
        give(group).start()
        return carry

    lax.fori_loop(0, groups, work, 0)
    deliver(groups - 1)
    ret_ref[groups - 1, each - 1] = done_ref[groups - 1, :, slot_rows(last)]

    def halves(step):
        return to_partner(near_ref.at[rows_of(step)], out_hbm.at[rows_of(step), near], half_send.at[step], half_recv.at[step])

    def keep(step):
        return pltpu.make_async_copy(near_ref.at[rows_of(step)], out_hbm.at[rows_of(step), near], keep_sem.at[step])

    def gather(group, carry):
        each_step(group, lambda step: ship_back(step).wait_recv())
        slots = iota((block, members), 1) + group * members

        def pick(step, carry):
            rows = rows_of(step)
            table = meta_ref[rows]
            dest = table.astype(jnp.int32)
            returned = ret_ref[group].reshape(members, half)
            one = dot_nn(jnp.where(slots == dest[:, 0:1], 1.0, 0.0).astype(BF16), returned)
            two = dot_nn(jnp.where(slots == dest[:, 1:2], 1.0, 0.0).astype(BF16), returned)
            result = acc_ref[rows] + (table[:, 2:3] * one + table[:, 3:4] * two)
            acc_ref[rows] = result

            @pl.when(group == groups - 1)
            def _():
                near_ref[rows] = result.astype(BF16)
                halves(step).start()
                keep(step).start()

            return carry

        lax.fori_loop(0, steps, pick, 0)
        return carry

    lax.fori_loop(0, groups, gather, 0)

    def finish(step, carry):
        halves(step).wait()
        keep(step).wait()
        return carry

    lax.fori_loop(0, steps, finish, 0)
    for step in range(last):
        ship(step).wait_send()
        ship_back(step).wait_send()

    def drain_pairs(group, carry):
        swap(group).wait_send()
        give(group).wait_send()
        return carry

    lax.fori_loop(0, groups, drain_pairs, 0)


def solution(mesh):
    ep_size = mesh.shape['ep']

    def local_fn(x, src_len, expert_idx, ln_gain, ln_bias, w_query, b_query, w_key, w_value, b_value, w_attn_out, b_attn_out, w_fc1, b_fc1, w_fc2, b_fc2, w_router, w_exp_in, b_exp_in, w_exp_out, b_exp_out):
        _, tokens, d_model = x.shape
        width = w_query.shape[2] * w_query.shape[3]
        num_experts = w_router.shape[1]
        local_experts, _, hidden = w_exp_in.shape
        cap = 2 * (-(-tokens // num_experts))
        half = d_model // 2
        groups = 4 if ep_size >= 16 else 2
        each = ep_size // groups
        block, chunk = min(256, tokens // 2), 16
        steps = tokens // block
        w_q, w_k, w_v = (jnp.transpose(w, (0, 2, 3, 1)).reshape(2, width, d_model) for w in (w_query, w_key, w_value))
        w_o = w_attn_out.reshape(2, width, d_model)
        idx = jnp.transpose(expert_idx, (0, 2, 1)).reshape(2, tokens)
        vmem = lambda *shape: pltpu.VMEM(shape, BF16)
        vmem32 = lambda *shape: pltpu.VMEM(shape, F32)
        dma = lambda *shape: pltpu.SemaphoreType.DMA(shape)
        far_away = pl.BlockSpec(memory_space=pl.ANY)
        rows = each * cap
        wide = vmem(groups, local_experts, rows, half)
        blocks = vmem(groups, each, local_experts, cap, half)
        result = pl.pallas_call(
            functools.partial(encoder_kernel, ep_size, groups, block, chunk),
            out_shape=jax.ShapeDtypeStruct((tokens, d_model), BF16),
            in_specs=[pl.BlockSpec(memory_space=pltpu.SMEM)] + [far_away] * 20,
            out_specs=far_away,
            scratch_shapes=[
                vmem(tokens, d_model), vmem(2, width, d_model), vmem(2, width, d_model), vmem(2, width, d_model), vmem(2, width, d_model), vmem(*w_fc1.shape), vmem(*w_fc2.shape), vmem32(*w_router.shape), vmem(*w_exp_in.shape), vmem(*w_exp_out.shape),
                pltpu.VMEM((2, tokens), jnp.int32), vmem32(4, d_model), vmem32(4, d_model), vmem32(width // 64, 2, 64), vmem32(width // 64, 2, 64), vmem32(2, d_model), vmem32(*b_fc1.shape), vmem32(*b_fc2.shape), vmem32(*b_exp_in.shape), vmem32(*b_exp_out.shape), dma(24), dma(steps),
                vmem(tokens, width), vmem(width // 64, tokens, 128), vmem(width // 64, tokens, 128), vmem(block, width), vmem32(block, tokens), vmem32(block, tokens), vmem(block, tokens), vmem(block, tokens), vmem32(block, 128), vmem(tokens, d_model), vmem(2, tokens, d_model), dma(3, steps), dma(3, steps),
                vmem(tokens, d_model), vmem32(tokens, num_experts), pltpu.VMEM((8, tokens), jnp.int32), vmem32(tokens, 128), blocks, wide, wide, vmem(local_experts, rows, half), wide, wide, wide, blocks,
                dma(ep_size), dma(ep_size), dma(groups), dma(groups), dma(groups), dma(groups), dma(ep_size), dma(ep_size), vmem32(tokens, half), vmem(tokens, half), dma(steps), dma(steps), dma(steps),
            ],
            compiler_params=pltpu.CompilerParams(collective_id=1, has_side_effects=True, vmem_limit_bytes=67043328),
        )(src_len, idx, x.reshape(tokens, d_model), ln_gain, ln_bias, w_q, w_k, w_v, w_o, jnp.transpose(b_query, (1, 0, 2)), jnp.transpose(b_value, (1, 0, 2)), b_attn_out, w_fc1, b_fc1, w_fc2, b_fc2, w_router, w_exp_in, b_exp_in, w_exp_out, b_exp_out)
        return result.reshape(1, tokens, d_model)

    in_specs = (P(('dp', 'ep'), None, None), P(('dp', 'ep')), P(('dp', 'ep'), None, None), P(), P(), P(None, None, 'tp', None), P(None, 'tp', None), P(None, None, 'tp', None), P(None, None, 'tp', None), P(None, 'tp', None), P(None, 'tp', None, None), P(), P(None, 'tp'), P('tp'), P('tp', None), P(), P(), P('ep', None, 'tp'), P('ep', 'tp'), P('ep', 'tp', None), P('ep', None))
    return jax.shard_map(local_fn, mesh=mesh, in_specs=in_specs, out_specs=P(('dp', 'ep'), None, None), check_vma=False)
```

```python
import functools

import jax
import jax.numpy as jnp
from jax import lax
from jax.experimental import pallas as pl
from jax.experimental.pallas import tpu as pltpu
from jax.sharding import PartitionSpec as P

LN_EPS = 1e-5
MESH = pl.DeviceIdType.MESH
F32 = jnp.float32
BF16 = jnp.bfloat16
MIN_LEN = 256


def dot_nn(a, b):
    return lax.dot_general(a, b, (((1,), (0,)), ((), ())), preferred_element_type=F32)


def dot_nt(a, b):
    return lax.dot_general(a, b, (((1,), (1,)), ((), ())), preferred_element_type=F32)


def layer_norm(block, gain, shift):
    block = block.astype(F32)
    centered = block - jnp.mean(block, axis=-1, keepdims=True)
    variance = jnp.mean(centered * centered, axis=-1, keepdims=True)
    return centered * lax.rsqrt(variance + LN_EPS) * gain + shift


def iota(shape, axis):
    return lax.broadcasted_iota(jnp.int32, shape, axis)


def send_order(ep_size):
    if ep_size != 64:
        return [(step,) for step in range(1, ep_size)] + [(0,)]

    def at(axis, value, rest):
        return tuple(rest[:axis]) + (value,) + tuple(rest[axis:])

    def both(offset):
        return [offset, tuple(-v % 4 for v in offset)]

    order = [o for signs in ((1, 1, 1), (1, 1, 3), (1, 3, 1), (3, 1, 1)) for o in both(signs)]
    for axis in range(3):
        for rest in ((1, 1), (1, 3)):
            order += both(at(axis, 2, rest)) + both(at(axis, 0, rest))
    for axis in range(3):
        order += both(at(axis, 1, (2, 2))) + both(at(axis, 1, (0, 0)))
    for axis in range(3):
        order += [at(axis, 2, (0, 0)), at(axis, 0, (2, 2))]
    order += [(2, 2, 2)]
    order += both((2, 1, 0)) + both((0, 2, 1)) + both((1, 0, 2)) + both((2, 0, 1)) + both((1, 2, 0)) + both((0, 1, 2))
    return order + [(0, 0, 0)]


def peer(ep_size, me, offset, sign):
    if ep_size != 64:
        return lax.rem(me + ep_size + sign * offset[0], ep_size)
    z, y, x = me // 16, lax.rem(me // 4, 4), lax.rem(me, 4)
    dz, dy, dx = ((sign * v) % 4 for v in offset)
    return lax.rem(z + dz, 4) * 16 + lax.rem(y + dy, 4) * 4 + lax.rem(x + dx, 4)


def order_place(ep_size, me, device):
    order = send_order(ep_size)
    if ep_size != 64:
        delta = device - me
        delta = jnp.where(delta < 0, delta + ep_size, delta)
        codes = [offset[0] for offset in order]
    else:
        z, y, x = me // 16, lax.rem(me // 4, 4), lax.rem(me, 4)
        delta = ((((device >> 4) - z) & 3) << 4) + (((((device >> 2) & 3) - y) & 3) << 2) + (((device & 3) - x) & 3)
        codes = [16 * dz + 4 * dy + dx for dz, dy, dx in order]
    place = jnp.zeros_like(device)
    for index, code in enumerate(codes):
        place = jnp.where(delta == code, index, place)
    return place


def encoder_kernel(ep_size, groups, block, chunk, len_ref, idx_hbm, x_hbm, gain_hbm, shift_hbm, wq_hbm, wk_hbm, wv_hbm, wo_hbm, bq_hbm, bv_hbm, bo_hbm, f1_hbm, fb1_hbm, f2_hbm, fb2_hbm, wr_hbm, e1_hbm, eb1_hbm, e2_hbm, eb2_hbm, out_hbm,
                   hid_ref, wq_ref, wk_ref, wv_ref, wo_ref, f1_ref, f2_ref, wr_ref, e1_ref, e2_ref, idx_ref, gain_ref, shift_ref, bq_ref, bv_ref, bo_ref, fb1_ref, fb2_ref, eb1_ref, eb2_ref, load_sem, x_sem,
                   q_ref, kx_ref, vx_ref, ctx_ref, s_even, s_odd, p_even, p_odd, head_ref, part_ref, recv_ref, part_send, part_recv,
                   norm_ref, logit_ref, dest_ref, meta_ref, disp_ref, mine_ref, other_ref, keep_ref, give_ref, take_ref, done_ref, ret_ref,
                   ship_send, ship_recv, swap_send, swap_recv, give_send, give_recv, back_send, back_recv, acc_ref, near_ref, keep_sem, half_send, half_recv, hot_ref):
    me, core = lax.axis_index('ep'), lax.axis_index('tp')
    tokens, d_model = hid_ref.shape
    steps = tokens // block
    width = q_ref.shape[1]
    local_experts, cap, half = disp_ref.shape[2:]
    experts = wr_ref.shape[1]
    each = ep_size // groups
    near = pl.ds(pl.multiple_of(core * half, half), half)
    far = pl.ds(pl.multiple_of((1 - core) * half, half), half)
    barrier = pltpu.get_barrier_semaphore()

    def rows_of(step):
        return pl.ds(pl.multiple_of(step * block, block), block)

    def to_partner(src, dst, send_sem, recv_sem):
        return pltpu.make_async_remote_copy(src_ref=src, dst_ref=dst, send_sem=send_sem, recv_sem=recv_sem, device_id={'tp': 1 - core}, device_id_type=MESH)

    def x_copy(step):
        return pltpu.make_async_copy(x_hbm.at[rows_of(step)], hid_ref.at[rows_of(step)], x_sem.at[step])

    loads = {}

    def load(name, src, dst):
        loads[name] = pltpu.make_async_copy(src, dst, load_sem.at[len(loads)])
        loads[name].start()

    def loaded(*names):
        for name in names:
            loads[name].wait()

    for step in range(steps):
        x_copy(step).start()
    load('gain', gain_hbm, gain_ref)
    load('shift', shift_hbm, shift_ref)
    load('q0', wq_hbm.at[0], wq_ref.at[0])
    load('k0', wk_hbm.at[0], wk_ref.at[0])
    load('v0', wv_hbm.at[0], wv_ref.at[0])
    load('bq', bq_hbm, bq_ref)
    load('bv', bv_hbm, bv_ref)
    order = send_order(ep_size)
    last = ep_size - 1
    for offset in order[:last]:
        pl.semaphore_signal(barrier, inc=1, device_id={'ep': peer(ep_size, me, offset, 1)}, device_id_type=MESH)
    pl.semaphore_signal(barrier, inc=1, device_id={'tp': 1 - core}, device_id_type=MESH)

    def exchange(stage, step):
        return to_partner(part_ref.at[rows_of(step)], recv_ref.at[stage % 2, rows_of(step)], part_send.at[stage, step], part_recv.at[stage, step])

    def two_by_two(await_step, act):
        def body(pair, carry):
            for step in (2 * pair, 2 * pair + 1):
                await_step(step)
            for step in (2 * pair, 2 * pair + 1):
                act(step)
            return carry

        lax.fori_loop(0, steps // 2, body, 0)

    def absorb(stage, step, bias):
        total = part_ref[rows_of(step)].astype(F32) + recv_ref[stage % 2, rows_of(step)].astype(F32)
        hidden = (hid_ref[rows_of(step)].astype(F32) + total + bias).astype(BF16)
        hid_ref[rows_of(step)] = hidden
        return hidden

    lane = iota((2 * block, 128), 1)

    def rows_of_pair(pair):
        return pl.ds(pl.multiple_of(2 * pair * block, 2 * block), 2 * block)

    key_ok = iota((chunk, tokens - MIN_LEN), 1) + MIN_LEN < len_ref[0] if tokens > MIN_LEN else None

    def softmax(s_ref, p_ref):
        for start in range(0, block, chunk):
            scores = s_ref[start:start + chunk]
            if key_ok is not None:
                scores = jnp.concatenate([scores[:, :MIN_LEN], jnp.where(key_ok, scores[:, MIN_LEN:], -1e30)], axis=1)
            weights = jnp.exp(scores - jnp.max(scores, axis=-1, keepdims=True))
            scale = 1.0 / jnp.sum(weights, axis=-1, keepdims=True)
            p_ref[start:start + chunk] = (weights * scale).astype(BF16)

    def project(layer, pair, normed):
        rows = rows_of_pair(pair)
        bias_q, bias_v = (jnp.concatenate([ref[head, layer:layer + 1] for head in range(width // 64)], axis=1) for ref in (bq_ref, bv_ref))
        query = (dot_nt(normed, wq_ref[layer]) + bias_q).astype(BF16)
        q_ref[rows] = (query.astype(F32) * 0.125).astype(BF16)
        keys = dot_nt(normed, wk_ref[layer])
        values = dot_nt(normed, wv_ref[layer]) + bias_v
        for head in range(width // 64):
            lanes = slice(128 * (head // 2), 128 * (head // 2) + 128)
            mine = (lane < 64) if head % 2 == 0 else (lane >= 64)
            kx_ref[head, rows] = jnp.where(mine, keys[:, lanes], 0.0).astype(BF16)
            vx_ref[head, rows] = jnp.where(mine, values[:, lanes], 0.0).astype(BF16)

    def attend(layer, stage):
        heads = width // 64
        s_refs, p_refs = (s_even, s_odd), (p_even, p_odd)

        def score(rows, head):
            lanes = slice(128 * (head // 2), 128 * (head // 2) + 128)
            s_refs[head % 2][...] = dot_nt(q_ref[rows, lanes], kx_ref[head])

        def weigh(head):
            lanes = slice(128 * (head // 2), 128 * (head // 2) + 128)
            mixed = dot_nn(p_refs[head % 2][...], vx_ref[head])
            if head % 2 == 0:
                head_ref[...] = mixed
            else:
                ctx_ref[:, lanes] = (head_ref[...] + mixed).astype(BF16)

        def body(step, carry):
            rows = rows_of(step)
            score(rows, 0)
            for head in range(heads + 1):
                if head + 1 < heads:
                    score(rows, head + 1)
                if head > 0:
                    weigh(head - 1)
                if head < heads:
                    softmax(s_refs[head % 2], p_refs[head % 2])
            part_ref[rows] = dot_nn(ctx_ref[...], wo_ref[layer]).astype(BF16)
            exchange(stage, step).start()
            return carry

        lax.fori_loop(0, steps, body, 0, unroll=2)

    def normed_hidden(hidden, norm):
        return layer_norm(hidden, gain_ref[norm:norm + 1], shift_ref[norm:norm + 1]).astype(BF16)

    loaded('gain', 'shift', 'bq', 'bv', 'q0', 'k0', 'v0')
    load('o', wo_hbm, wo_ref)
    load('bo', bo_hbm, bo_ref)
    load('f1', f1_hbm, f1_ref)
    load('fb1', fb1_hbm, fb1_ref)
    load('f2', f2_hbm, f2_ref)
    load('fb2', fb2_hbm, fb2_ref)
    for step in range(steps):
        x_copy(step).wait()
    for pair in range(steps // 2):
        project(0, pair, normed_hidden(hid_ref[rows_of_pair(pair)], 0))
    loaded('o', 'bo', 'f1', 'fb1', 'f2', 'fb2')
    load('q1', wq_hbm.at[1], wq_ref.at[1])
    load('k1', wk_hbm.at[1], wk_ref.at[1])
    load('v1', wv_hbm.at[1], wv_ref.at[1])
    load('idx', idx_hbm, idx_ref)
    load('r', wr_hbm, wr_ref)
    load('e1', e1_hbm, e1_ref)
    load('eb1', eb1_hbm, eb1_ref)
    load('e2', e2_hbm, e2_ref)
    load('eb2', eb2_hbm, eb2_ref)
    pl.semaphore_wait(barrier, ep_size)
    attend(0, 0)

    def feed(pair, carry):
        for step in (2 * pair, 2 * pair + 1):
            exchange(0, step).wait()
        normed = jnp.concatenate([normed_hidden(absorb(0, step, bo_ref[0:1]), 1) for step in (2 * pair, 2 * pair + 1)], axis=0)
        inner = jnp.maximum(dot_nn(normed, f1_ref[...]) + fb1_ref[...].reshape(1, -1), 0.0).astype(BF16)
        part_ref[rows_of_pair(pair)] = dot_nn(inner, f2_ref[...]).astype(BF16)
        for step in (2 * pair, 2 * pair + 1):
            exchange(1, step).start()
        return carry

    lax.fori_loop(0, steps // 2, feed, 0)
    loaded('q1', 'k1', 'v1')

    def second_project(pair, carry):
        both = (2 * pair, 2 * pair + 1)
        for step in both:
            exchange(1, step).wait()
        project(1, pair, jnp.concatenate([normed_hidden(absorb(1, step, fb2_ref[...].reshape(1, -1)), 2) for step in both], axis=0))
        return carry

    lax.fori_loop(0, steps // 2, second_project, 0)
    attend(1, 2)
    loaded('idx', 'r')

    valid = iota((1, tokens), 1) < len_ref[0]
    first, second = idx_ref[0:1], idx_ref[1:2]
    expert = iota((experts, tokens), 0)
    hot_first = jnp.where((expert == first) & valid, 1.0, 0.0)
    hot_second = jnp.where((expert == second) & valid, 1.0, 0.0)
    earlier = jnp.where(iota((tokens, tokens), 0) < iota((tokens, tokens), 1), 1.0, 0.0).astype(BF16)
    rank_first = dot_nn(hot_first.astype(BF16), earlier)
    rank_second = dot_nn(hot_second.astype(BF16), earlier) + jnp.sum(hot_first, axis=1, keepdims=True)
    slot_first = jnp.sum(rank_first * hot_first, axis=0, keepdims=True).astype(jnp.int32)
    slot_second = jnp.sum(rank_second * hot_second, axis=0, keepdims=True).astype(jnp.int32)

    choice, slot = idx_ref[...], jnp.concatenate([slot_first, slot_second], axis=0)
    home = ((order_place(ep_size, me, choice >> 1) << 1) + (choice & 1)) * cap + slot
    dest_ref[0:2] = jnp.where(valid & (slot < cap), home, experts * cap)
    router = wr_ref[...].astype(BF16)

    def settle(step):
        normed = normed_hidden(absorb(2, step, bo_ref[1:2]), 3)
        norm_ref[rows_of(step)] = normed
        logit_ref[rows_of(step)] = dot_nn(normed, router)

    two_by_two(lambda step: exchange(2, step).wait(), settle)

    def slot_rows(step):
        return pl.ds(step % each * cap, cap)

    def ship(step):
        return pltpu.make_async_remote_copy(src_ref=disp_ref.at[step // each, step % each], dst_ref=mine_ref.at[step // each, :, slot_rows(step)], send_sem=ship_send.at[step], recv_sem=ship_recv.at[step], device_id={'ep': peer(ep_size, me, order[step], 1)}, device_id_type=MESH)

    def ship_back(step):
        return pltpu.make_async_remote_copy(src_ref=done_ref.at[step // each, :, slot_rows(step)], dst_ref=ret_ref.at[step // each, step % each], send_sem=back_send.at[step], recv_sem=back_recv.at[step], device_id={'ep': peer(ep_size, me, order[step], -1)}, device_id_type=MESH)

    def swap(group):
        return to_partner(mine_ref.at[group], other_ref.at[group], swap_send.at[group], swap_recv.at[group])

    def give(group, expert):
        return to_partner(give_ref.at[group, expert], take_ref.at[group, expert], give_send.at[group, expert], give_recv.at[group, expert])

    def each_step(group, act):
        for index in range(groups):
            @pl.when(group == index)
            def _(index=index):
                for step in range(index * each, min((index + 1) * each, last)):
                    act(step)

    members = each * local_experts * cap

    def scatter(group, carry):
        slots = iota((members, tokens), 0) + group * members
        taken = jnp.where((slots == dest_ref[0:1]) | (slots == dest_ref[1:2]), 1.0, 0.0).astype(BF16)
        disp_ref[group] = dot_nn(taken, norm_ref[:, near]).astype(BF16).reshape(each, local_experts, cap, half)
        each_step(group, lambda step: ship(step).start())
        return carry

    lax.fori_loop(0, groups, scatter, 0)
    mine_ref[groups - 1, :, slot_rows(last)] = disp_ref[groups - 1, each - 1]

    row_id = iota((128, tokens), 0)
    packed = jnp.where(row_id == 0, dest_ref[0:1], jnp.where(row_id == 1, dest_ref[1:2], jnp.where(row_id == 2, first, second)))
    meta_ref[...] = packed.astype(F32).T
    column = iota((block, experts), 1).astype(F32)
    spot = iota((block, 128), 1)
    slots = iota((block, members), 1)

    def gate(step, carry):
        table, logits = meta_ref[rows_of(step)], logit_ref[rows_of(step)]
        logit_first = jnp.sum(jnp.where(column == table[:, 2:3], logits, 0.0), axis=1, keepdims=True)
        logit_second = jnp.sum(jnp.where(column == table[:, 3:4], logits, 0.0), axis=1, keepdims=True)
        gate_first = jax.nn.sigmoid(logit_first - logit_second)
        gate_second = jax.nn.sigmoid(logit_second - logit_first)
        meta_ref[rows_of(step)] = jnp.where(spot == 2, gate_first, jnp.where(spot == 3, gate_second, table))
        acc_ref[rows_of(step)] = hid_ref[rows_of(step), near].astype(F32)
        dest = table.astype(jnp.int32)
        for group in range(groups):
            for choice in range(2):
                hot_ref[group, step, choice * block:(choice + 1) * block] = jnp.where(slots == dest[:, choice:choice + 1] - group * members, 1.0, 0.0).astype(BF16)
        return carry

    lax.fori_loop(0, steps, gate, 0)
    loaded('e1', 'eb1', 'e2', 'eb2')

    def deliver(group):
        for expert in range(local_experts):
            give(group, expert).wait_recv()
            total = keep_ref[expert].astype(F32) + take_ref[group, expert].astype(F32)
            done_ref[group, expert] = (total + eb2_ref[expert:expert + 1, near]).astype(BF16)
        each_step(group, lambda step: ship_back(step).start())

    def arrive(group):
        each_step(group, lambda step: ship(step).wait_recv())
        swap(group).start()

    def work(group, carry):
        swap(group).wait_recv()
        for expert in range(local_experts):
            inner = dot_nn(mine_ref[group, expert], e1_ref[expert, near]) + dot_nn(other_ref[group, expert], e1_ref[expert, far])
            inner = jnp.maximum(inner + eb1_ref[expert:expert + 1], 0.0).astype(BF16)
            give_ref[group, expert] = dot_nn(inner, e2_ref[expert, :, far]).astype(BF16)
            give(group, expert).start()
            keep_ref[expert] = dot_nn(inner, e2_ref[expert, :, near]).astype(BF16)
            if expert == 0:
                @pl.when((group > 0) & (group < groups - 1))
                def _():
                    arrive(group + 1)

        deliver(group)

        @pl.when(group == 0)
        def _():
            arrive(1)

        return carry

    arrive(0)
    lax.fori_loop(0, groups, work, 0)
    ret_ref[groups - 1, each - 1] = done_ref[groups - 1, :, slot_rows(last)]

    def halves(step):
        return to_partner(near_ref.at[rows_of(step)], out_hbm.at[rows_of(step), near], half_send.at[step], half_recv.at[step])

    def keep(step):
        return pltpu.make_async_copy(near_ref.at[rows_of(step)], out_hbm.at[rows_of(step), near], keep_sem.at[step])

    def pick(group, step):
        rows = rows_of(step)
        table = meta_ref[rows]
        picked = dot_nn(hot_ref[group, step], ret_ref[group].reshape(members, half))
        return acc_ref[rows] + (table[:, 2:3] * picked[:block] + table[:, 3:4] * picked[block:])

    def gather(group, carry):
        each_step(group, lambda step: ship_back(step).wait_recv())

        def body(step, carry):
            acc_ref[rows_of(step)] = pick(group, step)
            return carry

        lax.fori_loop(0, steps, body, 0, unroll=True)
        return carry

    lax.fori_loop(0, groups - 1, gather, 0)
    each_step(groups - 1, lambda step: ship_back(step).wait_recv())

    def complete(step, carry):
        near_ref[rows_of(step)] = pick(groups - 1, step).astype(BF16)
        halves(step).start()
        keep(step).start()
        return carry

    lax.fori_loop(0, steps, complete, 0, unroll=True)

    def finish(step, carry):
        halves(step).wait()
        keep(step).wait()
        return carry

    lax.fori_loop(0, steps, finish, 0)
    for step in range(last):
        ship(step).wait_send()
        ship_back(step).wait_send()

    def drain_pairs(group, carry):
        swap(group).wait_send()
        for expert in range(local_experts):
            give(group, expert).wait_send()
        return carry

    lax.fori_loop(0, groups, drain_pairs, 0)


def solution(mesh):
    ep_size = mesh.shape['ep']

    def local_fn(x, src_len, expert_idx, ln_gain, ln_bias, w_query, b_query, w_key, w_value, b_value, w_attn_out, b_attn_out, w_fc1, b_fc1, w_fc2, b_fc2, w_router, w_exp_in, b_exp_in, w_exp_out, b_exp_out):
        _, tokens, d_model = x.shape
        width = w_query.shape[2] * w_query.shape[3]
        num_experts = w_router.shape[1]
        local_experts, _, hidden = w_exp_in.shape
        cap = 2 * (-(-tokens // num_experts))
        half = d_model // 2
        groups = 4 if ep_size >= 16 else 2
        each = ep_size // groups
        block, chunk = min(256, tokens // 2), 16
        steps = tokens // block
        w_q, w_k, w_v = (jnp.transpose(w, (0, 2, 3, 1)).reshape(2, width, d_model) for w in (w_query, w_key, w_value))
        w_o = w_attn_out.reshape(2, width, d_model)
        idx = jnp.transpose(expert_idx, (0, 2, 1)).reshape(2, tokens)
        vmem = lambda *shape: pltpu.VMEM(shape, BF16)
        vmem32 = lambda *shape: pltpu.VMEM(shape, F32)
        dma = lambda *shape: pltpu.SemaphoreType.DMA(shape)
        far_away = pl.BlockSpec(memory_space=pl.ANY)
        rows = each * cap
        wide = vmem(groups, local_experts, rows, half)
        blocks = vmem(groups, each, local_experts, cap, half)
        result = pl.pallas_call(
            functools.partial(encoder_kernel, ep_size, groups, block, chunk),
            out_shape=jax.ShapeDtypeStruct((tokens, d_model), BF16),
            in_specs=[pl.BlockSpec(memory_space=pltpu.SMEM)] + [far_away] * 20,
            out_specs=far_away,
            scratch_shapes=[
                vmem(tokens, d_model), vmem(2, width, d_model), vmem(2, width, d_model), vmem(2, width, d_model), vmem(2, width, d_model), vmem(*w_fc1.shape), vmem(*w_fc2.shape), vmem32(*w_router.shape), vmem(*w_exp_in.shape), vmem(*w_exp_out.shape),
                pltpu.VMEM((2, tokens), jnp.int32), vmem32(4, d_model), vmem32(4, d_model), vmem32(width // 64, 2, 64), vmem32(width // 64, 2, 64), vmem32(2, d_model), vmem32(*b_fc1.shape), vmem32(*b_fc2.shape), vmem32(*b_exp_in.shape), vmem32(*b_exp_out.shape), dma(24), dma(steps),
                vmem(tokens, width), vmem(width // 64, tokens, 128), vmem(width // 64, tokens, 128), vmem(block, width), vmem32(block, tokens), vmem32(block, tokens), vmem(block, tokens), vmem(block, tokens), vmem32(block, 128), vmem(tokens, d_model), vmem(2, tokens, d_model), dma(3, steps), dma(3, steps),
                vmem(tokens, d_model), vmem32(tokens, num_experts), pltpu.VMEM((8, tokens), jnp.int32), vmem32(tokens, 128), blocks, wide, wide, vmem(local_experts, rows, half), wide, wide, wide, blocks,
                dma(ep_size), dma(ep_size), dma(groups), dma(groups), dma(groups, local_experts), dma(groups, local_experts), dma(ep_size), dma(ep_size), vmem32(tokens, half), vmem(tokens, half), dma(steps), dma(steps), dma(steps), vmem(groups, steps, 2 * block, each * local_experts * cap),
            ],
            compiler_params=pltpu.CompilerParams(collective_id=1, has_side_effects=True, vmem_limit_bytes=67043328),
        )(src_len, idx, x.reshape(tokens, d_model), ln_gain, ln_bias, w_q, w_k, w_v, w_o, jnp.transpose(b_query, (1, 0, 2)), jnp.transpose(b_value, (1, 0, 2)), b_attn_out, w_fc1, b_fc1, w_fc2, b_fc2, w_router, w_exp_in, b_exp_in, w_exp_out, b_exp_out)
        return result.reshape(1, tokens, d_model)

    in_specs = (P(('dp', 'ep'), None, None), P(('dp', 'ep')), P(('dp', 'ep'), None, None), P(), P(), P(None, None, 'tp', None), P(None, 'tp', None), P(None, None, 'tp', None), P(None, None, 'tp', None), P(None, 'tp', None), P(None, 'tp', None, None), P(), P(None, 'tp'), P('tp'), P('tp', None), P(), P(), P('ep', None, 'tp'), P('ep', 'tp'), P('ep', 'tp', None), P('ep', None))
    return jax.shard_map(local_fn, mesh=mesh, in_specs=in_specs, out_specs=P(('dp', 'ep'), None, None), check_vma=False)
```

```python
import functools

import jax
import jax.numpy as jnp
from jax import lax
from jax.experimental import pallas as pl
from jax.experimental.pallas import tpu as pltpu
from jax.sharding import PartitionSpec as P

LN_EPS = 1e-5
MESH = pl.DeviceIdType.MESH
F32 = jnp.float32
BF16 = jnp.bfloat16
MIN_LEN = 256


def dot_nn(a, b):
    return lax.dot_general(a, b, (((1,), (0,)), ((), ())), preferred_element_type=F32)


def dot_nt(a, b):
    return lax.dot_general(a, b, (((1,), (1,)), ((), ())), preferred_element_type=F32)


def layer_norm(block, gain, shift):
    block = block.astype(F32)
    centered = block - jnp.mean(block, axis=-1, keepdims=True)
    variance = jnp.mean(centered * centered, axis=-1, keepdims=True)
    return centered * lax.rsqrt(variance + LN_EPS) * gain + shift


def iota(shape, axis):
    return lax.broadcasted_iota(jnp.int32, shape, axis)


def send_order(ep_size):
    if ep_size != 64:
        return [(step,) for step in range(1, ep_size)] + [(0,)]

    def at(axis, value, rest):
        return tuple(rest[:axis]) + (value,) + tuple(rest[axis:])

    def both(offset):
        return [offset, tuple(-v % 4 for v in offset)]

    order = [o for signs in ((1, 1, 1), (1, 1, 3), (1, 3, 1), (3, 1, 1)) for o in both(signs)]
    for axis in range(3):
        for rest in ((1, 1), (1, 3)):
            order += both(at(axis, 2, rest)) + both(at(axis, 0, rest))
    for axis in range(3):
        order += both(at(axis, 1, (2, 2))) + both(at(axis, 1, (0, 0)))
    for axis in range(3):
        order += [at(axis, 2, (0, 0)), at(axis, 0, (2, 2))]
    order += [(2, 2, 2)]
    order += both((2, 1, 0)) + both((0, 2, 1)) + both((1, 0, 2)) + both((2, 0, 1)) + both((1, 2, 0)) + both((0, 1, 2))
    return order + [(0, 0, 0)]


def peer(ep_size, me, offset, sign):
    if ep_size != 64:
        return lax.rem(me + ep_size + sign * offset[0], ep_size)
    z, y, x = me // 16, lax.rem(me // 4, 4), lax.rem(me, 4)
    dz, dy, dx = ((sign * v) % 4 for v in offset)
    return lax.rem(z + dz, 4) * 16 + lax.rem(y + dy, 4) * 4 + lax.rem(x + dx, 4)


def order_place(ep_size, me, device):
    order = send_order(ep_size)
    if ep_size != 64:
        delta = device - me
        delta = jnp.where(delta < 0, delta + ep_size, delta)
        codes = [offset[0] for offset in order]
    else:
        z, y, x = me // 16, lax.rem(me // 4, 4), lax.rem(me, 4)
        delta = ((((device >> 4) - z) & 3) << 4) + (((((device >> 2) & 3) - y) & 3) << 2) + (((device & 3) - x) & 3)
        codes = [16 * dz + 4 * dy + dx for dz, dy, dx in order]
    place = jnp.zeros_like(device)
    for index, code in enumerate(codes):
        place = jnp.where(delta == code, index, place)
    return place


def encoder_kernel(ep_size, groups, block, chunk, len_ref, idx_hbm, x_hbm, gain_hbm, shift_hbm, wq_hbm, wk_hbm, wv_hbm, wo_hbm, bq_hbm, bv_hbm, bo_hbm, f1_hbm, fb1_hbm, f2_hbm, fb2_hbm, wr_hbm, e1_hbm, eb1_hbm, e2_hbm, eb2_hbm, out_hbm,
                   hid_ref, wq_ref, wk_ref, wv_ref, wo_ref, f1_ref, f2_ref, wr_ref, e1_ref, e2_ref, idx_ref, gain_ref, shift_ref, bq_ref, bv_ref, bo_ref, fb1_ref, fb2_ref, eb1_ref, eb2_ref, load_sem, x_sem,
                   q_ref, kx_ref, vx_ref, ctx_ref, s_even, s_odd, p_even, p_odd, head_ref, part_ref, recv_ref, part_send, part_recv,
                   norm_ref, logit_ref, dest_ref, meta_ref, disp_ref, mine_ref, other_ref, keep_ref, give_ref, take_ref, done_ref, ret_ref,
                   ship_send, ship_recv, swap_send, swap_recv, give_send, give_recv, back_send, back_recv, acc_ref, near_ref, keep_sem, half_send, half_recv, hot_ref):
    me, core = lax.axis_index('ep'), lax.axis_index('tp')
    tokens, d_model = hid_ref.shape
    steps = tokens // block
    width = q_ref.shape[1]
    local_experts, cap, half = disp_ref.shape[2:]
    experts = wr_ref.shape[1]
    each = ep_size // groups
    near = pl.ds(pl.multiple_of(core * half, half), half)
    far = pl.ds(pl.multiple_of((1 - core) * half, half), half)
    barrier = pltpu.get_barrier_semaphore()

    def rows_of(step):
        return pl.ds(pl.multiple_of(step * block, block), block)

    def to_partner(src, dst, send_sem, recv_sem):
        return pltpu.make_async_remote_copy(src_ref=src, dst_ref=dst, send_sem=send_sem, recv_sem=recv_sem, device_id={'tp': 1 - core}, device_id_type=MESH)

    def x_copy(step):
        return pltpu.make_async_copy(x_hbm.at[rows_of(step)], hid_ref.at[rows_of(step)], x_sem.at[step])

    loads = {}

    def load(name, src, dst):
        loads[name] = pltpu.make_async_copy(src, dst, load_sem.at[len(loads)])
        loads[name].start()

    def loaded(*names):
        for name in names:
            loads[name].wait()

    for step in range(steps):
        x_copy(step).start()
    load('gain', gain_hbm, gain_ref)
    load('shift', shift_hbm, shift_ref)
    load('q0', wq_hbm.at[0], wq_ref.at[0])
    load('k0', wk_hbm.at[0], wk_ref.at[0])
    load('v0', wv_hbm.at[0], wv_ref.at[0])
    load('bq', bq_hbm, bq_ref)
    load('bv', bv_hbm, bv_ref)
    order = send_order(ep_size)
    last = ep_size - 1
    for offset in order[:last]:
        pl.semaphore_signal(barrier, inc=1, device_id={'ep': peer(ep_size, me, offset, 1)}, device_id_type=MESH)
    pl.semaphore_signal(barrier, inc=1, device_id={'tp': 1 - core}, device_id_type=MESH)

    def exchange(stage, step):
        return to_partner(part_ref.at[rows_of(step)], recv_ref.at[stage % 2, rows_of(step)], part_send.at[stage, step], part_recv.at[stage, step])

    def two_by_two(await_step, act):
        def body(pair, carry):
            for step in (2 * pair, 2 * pair + 1):
                await_step(step)
            for step in (2 * pair, 2 * pair + 1):
                act(step)
            return carry

        lax.fori_loop(0, steps // 2, body, 0)

    def absorb(stage, step, bias):
        total = part_ref[rows_of(step)].astype(F32) + recv_ref[stage % 2, rows_of(step)].astype(F32)
        hidden = (hid_ref[rows_of(step)].astype(F32) + total + bias).astype(BF16)
        hid_ref[rows_of(step)] = hidden
        return hidden

    lane = iota((2 * block, 128), 1)

    def rows_of_pair(pair):
        return pl.ds(pl.multiple_of(2 * pair * block, 2 * block), 2 * block)

    key_ok = iota((chunk, tokens - MIN_LEN), 1) + MIN_LEN < len_ref[0] if tokens > MIN_LEN else None

    def softmax(s_ref, p_ref):
        for start in range(0, block, chunk):
            scores = s_ref[start:start + chunk]
            if key_ok is not None:
                scores = jnp.concatenate([scores[:, :MIN_LEN], jnp.where(key_ok, scores[:, MIN_LEN:], -1e30)], axis=1)
            weights = jnp.exp(scores - jnp.max(scores, axis=-1, keepdims=True))
            scale = 1.0 / jnp.sum(weights, axis=-1, keepdims=True)
            p_ref[start:start + chunk] = (weights * scale).astype(BF16)

    def project(layer, pair, normed):
        rows = rows_of_pair(pair)
        bias_q, bias_v = (jnp.concatenate([ref[head, layer:layer + 1] for head in range(width // 64)], axis=1) for ref in (bq_ref, bv_ref))
        query = (dot_nt(normed, wq_ref[layer]) + bias_q).astype(BF16)
        q_ref[rows] = (query.astype(F32) * 0.125).astype(BF16)
        keys = dot_nt(normed, wk_ref[layer])
        values = dot_nt(normed, wv_ref[layer]) + bias_v
        for head in range(width // 64):
            lanes = slice(128 * (head // 2), 128 * (head // 2) + 128)
            mine = (lane < 64) if head % 2 == 0 else (lane >= 64)
            kx_ref[head, rows] = jnp.where(mine, keys[:, lanes], 0.0).astype(BF16)
            vx_ref[head, rows] = jnp.where(mine, values[:, lanes], 0.0).astype(BF16)

    def attend(layer, stage):
        heads = width // 64
        s_refs, p_refs = (s_even, s_odd), (p_even, p_odd)

        def score(rows, head):
            lanes = slice(128 * (head // 2), 128 * (head // 2) + 128)
            s_refs[head % 2][...] = dot_nt(q_ref[rows, lanes], kx_ref[head])

        def weigh(head):
            lanes = slice(128 * (head // 2), 128 * (head // 2) + 128)
            mixed = dot_nn(p_refs[head % 2][...], vx_ref[head])
            if head % 2 == 0:
                head_ref[...] = mixed
            else:
                ctx_ref[:, lanes] = (head_ref[...] + mixed).astype(BF16)

        def body(step, carry):
            rows = rows_of(step)
            score(rows, 0)
            for head in range(heads + 1):
                if head + 1 < heads:
                    score(rows, head + 1)
                if head > 0:
                    weigh(head - 1)
                if head < heads:
                    softmax(s_refs[head % 2], p_refs[head % 2])
            part_ref[rows] = dot_nn(ctx_ref[...], wo_ref[layer]).astype(BF16)
            exchange(stage, step).start()
            return carry

        lax.fori_loop(0, steps, body, 0, unroll=2)

    def normed_hidden(hidden, norm):
        return layer_norm(hidden, gain_ref[norm:norm + 1], shift_ref[norm:norm + 1]).astype(BF16)

    loaded('gain', 'shift', 'bq', 'bv', 'q0', 'k0', 'v0')
    load('o', wo_hbm, wo_ref)
    load('bo', bo_hbm, bo_ref)
    load('f1', f1_hbm, f1_ref)
    load('fb1', fb1_hbm, fb1_ref)
    load('f2', f2_hbm, f2_ref)
    load('fb2', fb2_hbm, fb2_ref)
    for step in range(steps):
        x_copy(step).wait()
    for pair in range(steps // 2):
        project(0, pair, normed_hidden(hid_ref[rows_of_pair(pair)], 0))
    loaded('o', 'bo', 'f1', 'fb1', 'f2', 'fb2')
    load('q1', wq_hbm.at[1], wq_ref.at[1])
    load('k1', wk_hbm.at[1], wk_ref.at[1])
    load('v1', wv_hbm.at[1], wv_ref.at[1])
    load('idx', idx_hbm, idx_ref)
    load('r', wr_hbm, wr_ref)
    load('e1', e1_hbm, e1_ref)
    load('eb1', eb1_hbm, eb1_ref)
    load('e2', e2_hbm, e2_ref)
    load('eb2', eb2_hbm, eb2_ref)
    pl.semaphore_wait(barrier, ep_size)
    attend(0, 0)

    def feed(pair, carry):
        for step in (2 * pair, 2 * pair + 1):
            exchange(0, step).wait()
        normed = jnp.concatenate([normed_hidden(absorb(0, step, bo_ref[0:1]), 1) for step in (2 * pair, 2 * pair + 1)], axis=0)
        inner = jnp.maximum(dot_nn(normed, f1_ref[...]) + fb1_ref[...].reshape(1, -1), 0.0).astype(BF16)
        part_ref[rows_of_pair(pair)] = dot_nn(inner, f2_ref[...]).astype(BF16)
        for step in (2 * pair, 2 * pair + 1):
            exchange(1, step).start()
        return carry

    lax.fori_loop(0, steps // 2, feed, 0)
    loaded('q1', 'k1', 'v1')

    def second_project(pair, carry):
        both = (2 * pair, 2 * pair + 1)
        for step in both:
            exchange(1, step).wait()
        project(1, pair, jnp.concatenate([normed_hidden(absorb(1, step, fb2_ref[...].reshape(1, -1)), 2) for step in both], axis=0))
        return carry

    lax.fori_loop(0, steps // 2, second_project, 0)
    attend(1, 2)
    loaded('idx', 'r')

    valid = iota((1, tokens), 1) < len_ref[0]
    first, second = idx_ref[0:1], idx_ref[1:2]
    expert = iota((experts, tokens), 0)
    hot_first = jnp.where((expert == first) & valid, 1.0, 0.0)
    hot_second = jnp.where((expert == second) & valid, 1.0, 0.0)
    earlier = jnp.where(iota((tokens, tokens), 0) < iota((tokens, tokens), 1), 1.0, 0.0).astype(BF16)
    rank_first = dot_nn(hot_first.astype(BF16), earlier)
    rank_second = dot_nn(hot_second.astype(BF16), earlier) + jnp.sum(hot_first, axis=1, keepdims=True)
    slot_first = jnp.sum(rank_first * hot_first, axis=0, keepdims=True).astype(jnp.int32)
    slot_second = jnp.sum(rank_second * hot_second, axis=0, keepdims=True).astype(jnp.int32)

    choice, slot = idx_ref[...], jnp.concatenate([slot_first, slot_second], axis=0)
    home = ((order_place(ep_size, me, choice >> 1) << 1) + (choice & 1)) * cap + slot
    dest_ref[0:2] = jnp.where(valid & (slot < cap), home, experts * cap)
    router = wr_ref[...].astype(BF16)

    def settle(step):
        normed = normed_hidden(absorb(2, step, bo_ref[1:2]), 3)
        norm_ref[rows_of(step)] = normed
        logit_ref[rows_of(step)] = dot_nn(normed, router)

    two_by_two(lambda step: exchange(2, step).wait(), settle)

    def slot_rows(step):
        return pl.ds(step % each * cap, cap)

    def ship(step):
        return pltpu.make_async_remote_copy(src_ref=disp_ref.at[step // each, step % each], dst_ref=mine_ref.at[step // each, :, slot_rows(step)], send_sem=ship_send.at[step], recv_sem=ship_recv.at[step], device_id={'ep': peer(ep_size, me, order[step], 1)}, device_id_type=MESH)

    def ship_back(step):
        return pltpu.make_async_remote_copy(src_ref=done_ref.at[step // each, :, slot_rows(step)], dst_ref=ret_ref.at[step // each, step % each], send_sem=back_send.at[step], recv_sem=back_recv.at[step], device_id={'ep': peer(ep_size, me, order[step], -1)}, device_id_type=MESH)

    def swap(group):
        return to_partner(mine_ref.at[group], other_ref.at[group], swap_send.at[group], swap_recv.at[group])

    def give(group, expert):
        return to_partner(give_ref.at[group, expert], take_ref.at[group, expert], give_send.at[group, expert], give_recv.at[group, expert])

    def each_step(group, act, among=range(groups)):
        for index in among:
            @pl.when(group == index)
            def _(index=index):
                for step in range(index * each, min((index + 1) * each, last)):
                    act(step)

    members = each * local_experts * cap

    def scatter(group, carry):
        slots = iota((members, tokens), 0) + group * members
        taken = jnp.where((slots == dest_ref[0:1]) | (slots == dest_ref[1:2]), 1.0, 0.0).astype(BF16)
        disp_ref[group] = dot_nn(taken, norm_ref[:, near]).astype(BF16).reshape(each, local_experts, cap, half)
        each_step(group, lambda step: ship(step).start(), range(groups - 1))
        return carry

    lax.fori_loop(0, groups, scatter, 0)
    mine_ref[groups - 1, :, slot_rows(last)] = disp_ref[groups - 1, each - 1]

    row_id = iota((128, tokens), 0)
    packed = jnp.where(row_id == 0, dest_ref[0:1], jnp.where(row_id == 1, dest_ref[1:2], jnp.where(row_id == 2, first, second)))
    meta_ref[...] = packed.astype(F32).T
    column = iota((block, experts), 1).astype(F32)
    spot = iota((block, 128), 1)
    slots = iota((block, members), 1)

    def gate(step, carry):
        table, logits = meta_ref[rows_of(step)], logit_ref[rows_of(step)]
        logit_first = jnp.sum(jnp.where(column == table[:, 2:3], logits, 0.0), axis=1, keepdims=True)
        logit_second = jnp.sum(jnp.where(column == table[:, 3:4], logits, 0.0), axis=1, keepdims=True)
        gate_first = jax.nn.sigmoid(logit_first - logit_second)
        gate_second = jax.nn.sigmoid(logit_second - logit_first)
        meta_ref[rows_of(step)] = jnp.where(spot == 2, gate_first, jnp.where(spot == 3, gate_second, table))
        acc_ref[rows_of(step)] = hid_ref[rows_of(step), near].astype(F32)
        dest = table.astype(jnp.int32)
        for group in range(groups):
            for choice in range(2):
                hot_ref[group, step, choice * block:(choice + 1) * block] = jnp.where(slots == dest[:, choice:choice + 1] - group * members, 1.0, 0.0).astype(BF16)
        return carry

    lax.fori_loop(0, steps, gate, 0)
    loaded('e1', 'eb1', 'e2', 'eb2')

    def deliver(group):
        for expert in range(local_experts):
            give(group, expert).wait_recv()
            total = keep_ref[expert].astype(F32) + take_ref[group, expert].astype(F32)
            done_ref[group, expert] = (total + eb2_ref[expert:expert + 1, near]).astype(BF16)
        each_step(group, lambda step: ship_back(step).start())

    def arrive(group):
        each_step(group, lambda step: ship(step).wait_recv())
        swap(group).start()

    def work(group, carry):
        swap(group).wait_recv()

        @pl.when(group == 0)
        def _():
            for step in range((groups - 1) * each, last):
                ship(step).start()

        for expert in range(local_experts):
            inner = dot_nn(mine_ref[group, expert], e1_ref[expert, near]) + dot_nn(other_ref[group, expert], e1_ref[expert, far])
            inner = jnp.maximum(inner + eb1_ref[expert:expert + 1], 0.0).astype(BF16)
            give_ref[group, expert] = dot_nn(inner, e2_ref[expert, :, far]).astype(BF16)
            give(group, expert).start()
            keep_ref[expert] = dot_nn(inner, e2_ref[expert, :, near]).astype(BF16)
            if expert == 0:
                @pl.when((group > 0) & (group < groups - 1))
                def _():
                    arrive(group + 1)

        deliver(group)

        @pl.when(group == 0)
        def _():
            arrive(1)

        return carry

    arrive(0)
    lax.fori_loop(0, groups, work, 0)
    ret_ref[groups - 1, each - 1] = done_ref[groups - 1, :, slot_rows(last)]

    def halves(step):
        return to_partner(near_ref.at[rows_of(step)], out_hbm.at[rows_of(step), near], half_send.at[step], half_recv.at[step])

    def keep(step):
        return pltpu.make_async_copy(near_ref.at[rows_of(step)], out_hbm.at[rows_of(step), near], keep_sem.at[step])

    def pick(group, step):
        rows = rows_of(step)
        table = meta_ref[rows]
        picked = dot_nn(hot_ref[group, step], ret_ref[group].reshape(members, half))
        return acc_ref[rows] + (table[:, 2:3] * picked[:block] + table[:, 3:4] * picked[block:])

    def gather(group, carry):
        each_step(group, lambda step: ship_back(step).wait_recv())

        def body(step, carry):
            acc_ref[rows_of(step)] = pick(group, step)
            return carry

        lax.fori_loop(0, steps, body, 0, unroll=True)
        return carry

    lax.fori_loop(0, groups - 1, gather, 0)
    each_step(groups - 1, lambda step: ship_back(step).wait_recv())

    def complete(step, carry):
        near_ref[rows_of(step)] = pick(groups - 1, step).astype(BF16)
        halves(step).start()
        keep(step).start()
        return carry

    lax.fori_loop(0, steps, complete, 0, unroll=2)

    def finish(step, carry):
        halves(step).wait()
        keep(step).wait()
        return carry

    lax.fori_loop(0, steps, finish, 0)
    for step in range(last):
        ship(step).wait_send()
        ship_back(step).wait_send()

    def drain_pairs(group, carry):
        swap(group).wait_send()
        for expert in range(local_experts):
            give(group, expert).wait_send()
        return carry

    lax.fori_loop(0, groups, drain_pairs, 0)


def solution(mesh):
    ep_size = mesh.shape['ep']

    def local_fn(x, src_len, expert_idx, ln_gain, ln_bias, w_query, b_query, w_key, w_value, b_value, w_attn_out, b_attn_out, w_fc1, b_fc1, w_fc2, b_fc2, w_router, w_exp_in, b_exp_in, w_exp_out, b_exp_out):
        _, tokens, d_model = x.shape
        width = w_query.shape[2] * w_query.shape[3]
        num_experts = w_router.shape[1]
        local_experts, _, hidden = w_exp_in.shape
        cap = 2 * (-(-tokens // num_experts))
        half = d_model // 2
        groups = 4 if ep_size >= 16 else 2
        each = ep_size // groups
        block, chunk = min(256, tokens // 2), 16
        steps = tokens // block
        w_q, w_k, w_v = (jnp.transpose(w, (0, 2, 3, 1)).reshape(2, width, d_model) for w in (w_query, w_key, w_value))
        w_o = w_attn_out.reshape(2, width, d_model)
        idx = jnp.transpose(expert_idx, (0, 2, 1)).reshape(2, tokens)
        vmem = lambda *shape: pltpu.VMEM(shape, BF16)
        vmem32 = lambda *shape: pltpu.VMEM(shape, F32)
        dma = lambda *shape: pltpu.SemaphoreType.DMA(shape)
        far_away = pl.BlockSpec(memory_space=pl.ANY)
        rows = each * cap
        wide = vmem(groups, local_experts, rows, half)
        blocks = vmem(groups, each, local_experts, cap, half)
        result = pl.pallas_call(
            functools.partial(encoder_kernel, ep_size, groups, block, chunk),
            out_shape=jax.ShapeDtypeStruct((tokens, d_model), BF16),
            in_specs=[pl.BlockSpec(memory_space=pltpu.SMEM)] + [far_away] * 20,
            out_specs=far_away,
            scratch_shapes=[
                vmem(tokens, d_model), vmem(2, width, d_model), vmem(2, width, d_model), vmem(2, width, d_model), vmem(2, width, d_model), vmem(*w_fc1.shape), vmem(*w_fc2.shape), vmem32(*w_router.shape), vmem(*w_exp_in.shape), vmem(*w_exp_out.shape),
                pltpu.VMEM((2, tokens), jnp.int32), vmem32(4, d_model), vmem32(4, d_model), vmem32(width // 64, 2, 64), vmem32(width // 64, 2, 64), vmem32(2, d_model), vmem32(*b_fc1.shape), vmem32(*b_fc2.shape), vmem32(*b_exp_in.shape), vmem32(*b_exp_out.shape), dma(24), dma(steps),
                vmem(tokens, width), vmem(width // 64, tokens, 128), vmem(width // 64, tokens, 128), vmem(block, width), vmem32(block, tokens), vmem32(block, tokens), vmem(block, tokens), vmem(block, tokens), vmem32(block, 128), vmem(tokens, d_model), vmem(2, tokens, d_model), dma(3, steps), dma(3, steps),
                vmem(tokens, d_model), vmem32(tokens, num_experts), pltpu.VMEM((8, tokens), jnp.int32), vmem32(tokens, 128), blocks, wide, wide, vmem(local_experts, rows, half), wide, wide, wide, blocks,
                dma(ep_size), dma(ep_size), dma(groups), dma(groups), dma(groups, local_experts), dma(groups, local_experts), dma(ep_size), dma(ep_size), vmem32(tokens, half), vmem(tokens, half), dma(steps), dma(steps), dma(steps), vmem(groups, steps, 2 * block, each * local_experts * cap),
            ],
            compiler_params=pltpu.CompilerParams(collective_id=1, has_side_effects=True, vmem_limit_bytes=67043328),
        )(src_len, idx, x.reshape(tokens, d_model), ln_gain, ln_bias, w_q, w_k, w_v, w_o, jnp.transpose(b_query, (1, 0, 2)), jnp.transpose(b_value, (1, 0, 2)), b_attn_out, w_fc1, b_fc1, w_fc2, b_fc2, w_router, w_exp_in, b_exp_in, w_exp_out, b_exp_out)
        return result.reshape(1, tokens, d_model)

    in_specs = (P(('dp', 'ep'), None, None), P(('dp', 'ep')), P(('dp', 'ep'), None, None), P(), P(), P(None, None, 'tp', None), P(None, 'tp', None), P(None, None, 'tp', None), P(None, None, 'tp', None), P(None, 'tp', None), P(None, 'tp', None, None), P(), P(None, 'tp'), P('tp'), P('tp', None), P(), P(), P('ep', None, 'tp'), P('ep', 'tp'), P('ep', 'tp', None), P('ep', None))
    return jax.shard_map(local_fn, mesh=mesh, in_specs=in_specs, out_specs=P(('dp', 'ep'), None, None), check_vma=False)
```

```python
import functools

import jax
import jax.numpy as jnp
from jax import lax
from jax.experimental import pallas as pl
from jax.experimental.pallas import tpu as pltpu
from jax.sharding import PartitionSpec as P

LN_EPS = 1e-5
MESH = pl.DeviceIdType.MESH
F32 = jnp.float32
BF16 = jnp.bfloat16
MIN_LEN = 256


def dot_nn(a, b):
    return lax.dot_general(a, b, (((1,), (0,)), ((), ())), preferred_element_type=F32)


def dot_nt(a, b):
    return lax.dot_general(a, b, (((1,), (1,)), ((), ())), preferred_element_type=F32)


def layer_norm(block, gain, shift):
    block = block.astype(F32)
    centered = block - jnp.mean(block, axis=-1, keepdims=True)
    variance = jnp.mean(centered * centered, axis=-1, keepdims=True)
    return centered * lax.rsqrt(variance + LN_EPS) * gain + shift


def iota(shape, axis):
    return lax.broadcasted_iota(jnp.int32, shape, axis)


def send_order(ep_size):
    if ep_size != 64:
        return [(step,) for step in range(1, ep_size)] + [(0,)]

    def at(axis, value, rest):
        return tuple(rest[:axis]) + (value,) + tuple(rest[axis:])

    def both(offset):
        return [offset, tuple(-v % 4 for v in offset)]

    order = [o for signs in ((1, 1, 1), (1, 1, 3), (1, 3, 1), (3, 1, 1)) for o in both(signs)]
    for axis in range(3):
        for rest in ((1, 1), (1, 3)):
            order += both(at(axis, 2, rest)) + both(at(axis, 0, rest))
    for axis in range(3):
        order += both(at(axis, 1, (2, 2))) + both(at(axis, 1, (0, 0)))
    for axis in range(3):
        order += [at(axis, 2, (0, 0)), at(axis, 0, (2, 2))]
    order += [(2, 2, 2)]
    order += both((2, 1, 0)) + both((0, 2, 1)) + both((1, 0, 2)) + both((2, 0, 1)) + both((1, 2, 0)) + both((0, 1, 2))
    return order + [(0, 0, 0)]


def peer(ep_size, me, offset, sign):
    if ep_size != 64:
        return lax.rem(me + ep_size + sign * offset[0], ep_size)
    z, y, x = me // 16, lax.rem(me // 4, 4), lax.rem(me, 4)
    dz, dy, dx = ((sign * v) % 4 for v in offset)
    return lax.rem(z + dz, 4) * 16 + lax.rem(y + dy, 4) * 4 + lax.rem(x + dx, 4)


def order_place(ep_size, me, device):
    order = send_order(ep_size)
    if ep_size != 64:
        delta = device - me
        delta = jnp.where(delta < 0, delta + ep_size, delta)
        codes = [offset[0] for offset in order]
    else:
        z, y, x = me // 16, lax.rem(me // 4, 4), lax.rem(me, 4)
        delta = ((((device >> 4) - z) & 3) << 4) + (((((device >> 2) & 3) - y) & 3) << 2) + (((device & 3) - x) & 3)
        codes = [16 * dz + 4 * dy + dx for dz, dy, dx in order]
    place = jnp.zeros_like(device)
    for index, code in enumerate(codes):
        place = jnp.where(delta == code, index, place)
    return place


def encoder_kernel(ep_size, groups, block, chunk, len_ref, idx_hbm, x_hbm, gain_hbm, shift_hbm, wq_hbm, wk_hbm, wv_hbm, wo_hbm, bq_hbm, bv_hbm, bo_hbm, f1_hbm, fb1_hbm, f2_hbm, fb2_hbm, wr_hbm, e1_hbm, eb1_hbm, e2_hbm, eb2_hbm, out_hbm,
                   hid_ref, wq_ref, wk_ref, wv_ref, wo_ref, f1_ref, f2_ref, wr_ref, e1_ref, e2_ref, idx_ref, gain_ref, shift_ref, bq_ref, bv_ref, bo_ref, fb1_ref, fb2_ref, eb1_ref, eb2_ref, load_sem, x_sem,
                   q_ref, kx_ref, vx_ref, ctx_ref, s_even, s_odd, p_even, p_odd, head_ref, part_ref, recv_ref, part_send, part_recv,
                   norm_ref, logit_ref, dest_ref, meta_ref, disp_ref, joint_ref, sum_ref, take_ref, done_ref, ret_ref,
                   ship_send, ship_recv, swap_send, swap_recv, give_send, give_recv, back_send, back_recv, acc_ref, near_ref, keep_sem, half_send, half_recv, hot_ref):
    me, core = lax.axis_index('ep'), lax.axis_index('tp')
    tokens, d_model = hid_ref.shape
    steps = tokens // block
    width = q_ref.shape[1]
    local_experts, cap, half = disp_ref.shape[2:]
    experts = wr_ref.shape[1]
    each = ep_size // groups
    near = pl.ds(pl.multiple_of(core * half, half), half)
    far = pl.ds(pl.multiple_of((1 - core) * half, half), half)
    barrier = pltpu.get_barrier_semaphore()

    def rows_of(step):
        return pl.ds(pl.multiple_of(step * block, block), block)

    def to_partner(src, dst, send_sem, recv_sem):
        return pltpu.make_async_remote_copy(src_ref=src, dst_ref=dst, send_sem=send_sem, recv_sem=recv_sem, device_id={'tp': 1 - core}, device_id_type=MESH)

    def x_copy(step):
        return pltpu.make_async_copy(x_hbm.at[rows_of(step)], hid_ref.at[rows_of(step)], x_sem.at[step])

    loads = {}

    def load(name, src, dst):
        loads[name] = pltpu.make_async_copy(src, dst, load_sem.at[len(loads)])
        loads[name].start()

    def loaded(*names):
        for name in names:
            loads[name].wait()

    for step in range(steps):
        x_copy(step).start()
    load('gain', gain_hbm, gain_ref)
    load('shift', shift_hbm, shift_ref)
    load('q0', wq_hbm.at[0], wq_ref.at[0])
    load('k0', wk_hbm.at[0], wk_ref.at[0])
    load('v0', wv_hbm.at[0], wv_ref.at[0])
    load('bq', bq_hbm, bq_ref)
    load('bv', bv_hbm, bv_ref)
    order = send_order(ep_size)
    last = ep_size - 1
    for offset in order[:last]:
        pl.semaphore_signal(barrier, inc=1, device_id={'ep': peer(ep_size, me, offset, 1)}, device_id_type=MESH)
    pl.semaphore_signal(barrier, inc=1, device_id={'tp': 1 - core}, device_id_type=MESH)

    def exchange(stage, step):
        return to_partner(part_ref.at[rows_of(step)], recv_ref.at[stage % 2, rows_of(step)], part_send.at[stage, step], part_recv.at[stage, step])

    def two_by_two(await_step, act):
        def body(pair, carry):
            for step in (2 * pair, 2 * pair + 1):
                await_step(step)
            for step in (2 * pair, 2 * pair + 1):
                act(step)
            return carry

        lax.fori_loop(0, steps // 2, body, 0)

    def absorb(stage, step, bias):
        total = part_ref[rows_of(step)].astype(F32) + recv_ref[stage % 2, rows_of(step)].astype(F32)
        hidden = (hid_ref[rows_of(step)].astype(F32) + total + bias).astype(BF16)
        hid_ref[rows_of(step)] = hidden
        return hidden

    lane = iota((2 * block, 128), 1)

    def rows_of_pair(pair):
        return pl.ds(pl.multiple_of(2 * pair * block, 2 * block), 2 * block)

    key_ok = iota((chunk, tokens - MIN_LEN), 1) + MIN_LEN < len_ref[0] if tokens > MIN_LEN else None

    def softmax(s_ref, p_ref):
        for start in range(0, block, chunk):
            scores = s_ref[start:start + chunk]
            if key_ok is not None:
                scores = jnp.concatenate([scores[:, :MIN_LEN], jnp.where(key_ok, scores[:, MIN_LEN:], -1e30)], axis=1)
            weights = jnp.exp(scores - jnp.max(scores, axis=-1, keepdims=True))
            scale = 1.0 / jnp.sum(weights, axis=-1, keepdims=True)
            p_ref[start:start + chunk] = (weights * scale).astype(BF16)

    def project(layer, pair, normed):
        rows = rows_of_pair(pair)
        bias_q, bias_v = (jnp.concatenate([ref[head, layer:layer + 1] for head in range(width // 64)], axis=1) for ref in (bq_ref, bv_ref))
        query = (dot_nt(normed, wq_ref[layer]) + bias_q).astype(BF16)
        q_ref[rows] = (query.astype(F32) * 0.125).astype(BF16)
        keys = dot_nt(normed, wk_ref[layer])
        values = dot_nt(normed, wv_ref[layer]) + bias_v
        for head in range(width // 64):
            lanes = slice(128 * (head // 2), 128 * (head // 2) + 128)
            mine = (lane < 64) if head % 2 == 0 else (lane >= 64)
            kx_ref[head, rows] = jnp.where(mine, keys[:, lanes], 0.0).astype(BF16)
            vx_ref[head, rows] = jnp.where(mine, values[:, lanes], 0.0).astype(BF16)

    def attend(layer, stage):
        heads = width // 64
        s_refs, p_refs = (s_even, s_odd), (p_even, p_odd)

        def score(rows, head):
            lanes = slice(128 * (head // 2), 128 * (head // 2) + 128)
            s_refs[head % 2][...] = dot_nt(q_ref[rows, lanes], kx_ref[head])

        def weigh(head):
            lanes = slice(128 * (head // 2), 128 * (head // 2) + 128)
            mixed = dot_nn(p_refs[head % 2][...], vx_ref[head])
            if head % 2 == 0:
                head_ref[...] = mixed
            else:
                ctx_ref[:, lanes] = (head_ref[...] + mixed).astype(BF16)

        def body(step, carry):
            rows = rows_of(step)
            score(rows, 0)
            for head in range(heads + 1):
                if head + 1 < heads:
                    score(rows, head + 1)
                if head > 0:
                    weigh(head - 1)
                if head < heads:
                    softmax(s_refs[head % 2], p_refs[head % 2])
            part_ref[rows] = dot_nn(ctx_ref[...], wo_ref[layer]).astype(BF16)
            exchange(stage, step).start()
            return carry

        lax.fori_loop(0, steps, body, 0, unroll=2)

    def normed_hidden(hidden, norm):
        return layer_norm(hidden, gain_ref[norm:norm + 1], shift_ref[norm:norm + 1]).astype(BF16)

    loaded('gain', 'shift', 'bq', 'bv', 'q0', 'k0', 'v0')
    load('o', wo_hbm, wo_ref)
    load('bo', bo_hbm, bo_ref)
    load('f1', f1_hbm, f1_ref)
    load('fb1', fb1_hbm, fb1_ref)
    load('f2', f2_hbm, f2_ref)
    load('fb2', fb2_hbm, fb2_ref)
    for step in range(steps):
        x_copy(step).wait()
    for pair in range(steps // 2):
        project(0, pair, normed_hidden(hid_ref[rows_of_pair(pair)], 0))
    loaded('o', 'bo', 'f1', 'fb1', 'f2', 'fb2')
    load('q1', wq_hbm.at[1], wq_ref.at[1])
    load('k1', wk_hbm.at[1], wk_ref.at[1])
    load('v1', wv_hbm.at[1], wv_ref.at[1])
    load('idx', idx_hbm, idx_ref)
    load('r', wr_hbm, wr_ref)
    load('e1', e1_hbm, e1_ref)
    load('eb1', eb1_hbm, eb1_ref)
    load('e2', e2_hbm, e2_ref)
    load('eb2', eb2_hbm, eb2_ref)
    pl.semaphore_wait(barrier, ep_size)
    attend(0, 0)

    def feed(pair, carry):
        for step in (2 * pair, 2 * pair + 1):
            exchange(0, step).wait()
        normed = jnp.concatenate([normed_hidden(absorb(0, step, bo_ref[0:1]), 1) for step in (2 * pair, 2 * pair + 1)], axis=0)
        inner = jnp.maximum(dot_nn(normed, f1_ref[...]) + fb1_ref[...].reshape(1, -1), 0.0).astype(BF16)
        part_ref[rows_of_pair(pair)] = dot_nn(inner, f2_ref[...]).astype(BF16)
        for step in (2 * pair, 2 * pair + 1):
            exchange(1, step).start()
        return carry

    lax.fori_loop(0, steps // 2, feed, 0)
    loaded('q1', 'k1', 'v1')

    def second_project(pair, carry):
        both = (2 * pair, 2 * pair + 1)
        for step in both:
            exchange(1, step).wait()
        project(1, pair, jnp.concatenate([normed_hidden(absorb(1, step, fb2_ref[...].reshape(1, -1)), 2) for step in both], axis=0))
        return carry

    lax.fori_loop(0, steps // 2, second_project, 0)
    attend(1, 2)
    loaded('idx', 'r')

    valid = iota((1, tokens), 1) < len_ref[0]
    first, second = idx_ref[0:1], idx_ref[1:2]
    expert = iota((experts, tokens), 0)
    hot_first = jnp.where((expert == first) & valid, 1.0, 0.0)
    hot_second = jnp.where((expert == second) & valid, 1.0, 0.0)
    earlier = jnp.where(iota((tokens, tokens), 0) < iota((tokens, tokens), 1), 1.0, 0.0).astype(BF16)
    rank_first = dot_nn(hot_first.astype(BF16), earlier)
    rank_second = dot_nn(hot_second.astype(BF16), earlier) + jnp.sum(hot_first, axis=1, keepdims=True)
    slot_first = jnp.sum(rank_first * hot_first, axis=0, keepdims=True).astype(jnp.int32)
    slot_second = jnp.sum(rank_second * hot_second, axis=0, keepdims=True).astype(jnp.int32)

    choice, slot = idx_ref[...], jnp.concatenate([slot_first, slot_second], axis=0)
    home = ((order_place(ep_size, me, choice >> 1) << 1) + (choice & 1)) * cap + slot
    dest_ref[0:2] = jnp.where(valid & (slot < cap), home, experts * cap)
    router = wr_ref[...].astype(BF16)

    def settle(step):
        normed = normed_hidden(absorb(2, step, bo_ref[1:2]), 3)
        norm_ref[rows_of(step)] = normed
        logit_ref[rows_of(step)] = dot_nn(normed, router)

    two_by_two(lambda step: exchange(2, step).wait(), settle)

    def slot_rows(step):
        return pl.ds(step % each * cap, cap)

    def ship(step):
        return pltpu.make_async_remote_copy(src_ref=disp_ref.at[step // each, step % each], dst_ref=joint_ref.at[step // each, :, slot_rows(step), near], send_sem=ship_send.at[step], recv_sem=ship_recv.at[step], device_id={'ep': peer(ep_size, me, order[step], 1)}, device_id_type=MESH)

    def ship_back(step):
        return pltpu.make_async_remote_copy(src_ref=done_ref.at[step // each, :, slot_rows(step)], dst_ref=ret_ref.at[step // each, step % each], send_sem=back_send.at[step], recv_sem=back_recv.at[step], device_id={'ep': peer(ep_size, me, order[step], -1)}, device_id_type=MESH)

    def swap(group):
        return to_partner(joint_ref.at[group, :, :, near], joint_ref.at[group, :, :, near], swap_send.at[group], swap_recv.at[group])

    def give(group, expert):
        return to_partner(sum_ref.at[group, expert, :, far], take_ref.at[group, expert], give_send.at[group, expert], give_recv.at[group, expert])

    def each_step(group, act):
        for index in range(groups):
            @pl.when(group == index)
            def _(index=index):
                for step in range(index * each, min((index + 1) * each, last)):
                    act(step)

    members = each * local_experts * cap

    def scatter(group, carry):
        slots = iota((members, tokens), 0) + group * members
        taken = jnp.where((slots == dest_ref[0:1]) | (slots == dest_ref[1:2]), 1.0, 0.0).astype(BF16)
        disp_ref[group] = dot_nn(taken, norm_ref[:, near]).astype(BF16).reshape(each, local_experts, cap, half)
        each_step(group, lambda step: ship(step).start())
        return carry

    lax.fori_loop(0, groups, scatter, 0)
    joint_ref[groups - 1, :, slot_rows(last), near] = disp_ref[groups - 1, each - 1]

    row_id = iota((128, tokens), 0)
    packed = jnp.where(row_id == 0, dest_ref[0:1], jnp.where(row_id == 1, dest_ref[1:2], jnp.where(row_id == 2, first, second)))
    meta_ref[...] = packed.astype(F32).T
    column = iota((block, experts), 1).astype(F32)
    spot = iota((block, 128), 1)
    slots = iota((block, members), 1)

    def gate(step, carry):
        table, logits = meta_ref[rows_of(step)], logit_ref[rows_of(step)]
        logit_first = jnp.sum(jnp.where(column == table[:, 2:3], logits, 0.0), axis=1, keepdims=True)
        logit_second = jnp.sum(jnp.where(column == table[:, 3:4], logits, 0.0), axis=1, keepdims=True)
        gate_first = jax.nn.sigmoid(logit_first - logit_second)
        gate_second = jax.nn.sigmoid(logit_second - logit_first)
        meta_ref[rows_of(step)] = jnp.where(spot == 2, gate_first, jnp.where(spot == 3, gate_second, table))
        acc_ref[rows_of(step)] = hid_ref[rows_of(step), near].astype(F32)
        dest = table.astype(jnp.int32)
        for group in range(groups):
            for choice in range(2):
                hot_ref[group, step, choice * block:(choice + 1) * block] = jnp.where(slots == dest[:, choice:choice + 1] - group * members, 1.0, 0.0).astype(BF16)
        return carry

    lax.fori_loop(0, steps, gate, 0)
    loaded('e1', 'eb1', 'e2', 'eb2')

    def deliver(group):
        for expert in range(local_experts):
            give(group, expert).wait_recv()
            total = sum_ref[group, expert, :, near].astype(F32) + take_ref[group, expert].astype(F32)
            done_ref[group, expert] = (total + eb2_ref[expert:expert + 1, near]).astype(BF16)
        each_step(group, lambda step: ship_back(step).start())

    def arrive(group):
        each_step(group, lambda step: ship(step).wait_recv())
        swap(group).start()

    def work(group, carry):
        swap(group).wait_recv()
        for expert in range(local_experts):
            inner = jnp.maximum(dot_nn(joint_ref[group, expert], e1_ref[expert]) + eb1_ref[expert:expert + 1], 0.0).astype(BF16)
            sum_ref[group, expert] = dot_nn(inner, e2_ref[expert]).astype(BF16)
            give(group, expert).start()
            if expert == 0:
                @pl.when((group > 0) & (group < groups - 1))
                def _():
                    arrive(group + 1)

        deliver(group)

        @pl.when(group == 0)
        def _():
            arrive(1)

        return carry

    arrive(0)
    lax.fori_loop(0, groups, work, 0)
    ret_ref[groups - 1, each - 1] = done_ref[groups - 1, :, slot_rows(last)]

    def halves(step):
        return to_partner(near_ref.at[rows_of(step)], out_hbm.at[rows_of(step), near], half_send.at[step], half_recv.at[step])

    def keep(step):
        return pltpu.make_async_copy(near_ref.at[rows_of(step)], out_hbm.at[rows_of(step), near], keep_sem.at[step])

    def pick(group, step):
        rows = rows_of(step)
        table = meta_ref[rows]
        picked = dot_nn(hot_ref[group, step], ret_ref[group].reshape(members, half))
        return acc_ref[rows] + (table[:, 2:3] * picked[:block] + table[:, 3:4] * picked[block:])

    def gather(group, carry):
        each_step(group, lambda step: ship_back(step).wait_recv())

        def body(step, carry):
            acc_ref[rows_of(step)] = pick(group, step)
            return carry

        lax.fori_loop(0, steps, body, 0, unroll=True)
        return carry

    lax.fori_loop(0, groups - 1, gather, 0)
    each_step(groups - 1, lambda step: ship_back(step).wait_recv())

    def complete(step, carry):
        near_ref[rows_of(step)] = pick(groups - 1, step).astype(BF16)
        halves(step).start()
        keep(step).start()
        return carry

    lax.fori_loop(0, steps, complete, 0, unroll=True)

    def finish(step, carry):
        halves(step).wait()
        keep(step).wait()
        return carry

    lax.fori_loop(0, steps, finish, 0)
    for step in range(last):
        ship(step).wait_send()
        ship_back(step).wait_send()

    def drain_pairs(group, carry):
        swap(group).wait_send()
        for expert in range(local_experts):
            give(group, expert).wait_send()
        return carry

    lax.fori_loop(0, groups, drain_pairs, 0)


def solution(mesh):
    ep_size = mesh.shape['ep']

    def local_fn(x, src_len, expert_idx, ln_gain, ln_bias, w_query, b_query, w_key, w_value, b_value, w_attn_out, b_attn_out, w_fc1, b_fc1, w_fc2, b_fc2, w_router, w_exp_in, b_exp_in, w_exp_out, b_exp_out):
        _, tokens, d_model = x.shape
        width = w_query.shape[2] * w_query.shape[3]
        num_experts = w_router.shape[1]
        local_experts, _, hidden = w_exp_in.shape
        cap = 2 * (-(-tokens // num_experts))
        half = d_model // 2
        groups = 4 if ep_size >= 16 else 2
        each = ep_size // groups
        block, chunk = min(256, tokens // 2), 16
        steps = tokens // block
        w_q, w_k, w_v = (jnp.transpose(w, (0, 2, 3, 1)).reshape(2, width, d_model) for w in (w_query, w_key, w_value))
        w_o = w_attn_out.reshape(2, width, d_model)
        idx = jnp.transpose(expert_idx, (0, 2, 1)).reshape(2, tokens)
        vmem = lambda *shape: pltpu.VMEM(shape, BF16)
        vmem32 = lambda *shape: pltpu.VMEM(shape, F32)
        dma = lambda *shape: pltpu.SemaphoreType.DMA(shape)
        far_away = pl.BlockSpec(memory_space=pl.ANY)
        rows = each * cap
        wide = vmem(groups, local_experts, rows, half)
        full = vmem(groups, local_experts, rows, d_model)
        blocks = vmem(groups, each, local_experts, cap, half)
        result = pl.pallas_call(
            functools.partial(encoder_kernel, ep_size, groups, block, chunk),
            out_shape=jax.ShapeDtypeStruct((tokens, d_model), BF16),
            in_specs=[pl.BlockSpec(memory_space=pltpu.SMEM)] + [far_away] * 20,
            out_specs=far_away,
            scratch_shapes=[
                vmem(tokens, d_model), vmem(2, width, d_model), vmem(2, width, d_model), vmem(2, width, d_model), vmem(2, width, d_model), vmem(*w_fc1.shape), vmem(*w_fc2.shape), vmem32(*w_router.shape), vmem(*w_exp_in.shape), vmem(*w_exp_out.shape),
                pltpu.VMEM((2, tokens), jnp.int32), vmem32(4, d_model), vmem32(4, d_model), vmem32(width // 64, 2, 64), vmem32(width // 64, 2, 64), vmem32(2, d_model), vmem32(*b_fc1.shape), vmem32(*b_fc2.shape), vmem32(*b_exp_in.shape), vmem32(*b_exp_out.shape), dma(24), dma(steps),
                vmem(tokens, width), vmem(width // 64, tokens, 128), vmem(width // 64, tokens, 128), vmem(block, width), vmem32(block, tokens), vmem32(block, tokens), vmem(block, tokens), vmem(block, tokens), vmem32(block, 128), vmem(tokens, d_model), vmem(2, tokens, d_model), dma(3, steps), dma(3, steps),
                vmem(tokens, d_model), vmem32(tokens, num_experts), pltpu.VMEM((8, tokens), jnp.int32), vmem32(tokens, 128), blocks, full, full, wide, wide, blocks,
                dma(ep_size), dma(ep_size), dma(groups), dma(groups), dma(groups, local_experts), dma(groups, local_experts), dma(ep_size), dma(ep_size), vmem32(tokens, half), vmem(tokens, half), dma(steps), dma(steps), dma(steps), vmem(groups, steps, 2 * block, each * local_experts * cap),
            ],
            compiler_params=pltpu.CompilerParams(collective_id=1, has_side_effects=True, vmem_limit_bytes=67043328),
        )(src_len, idx, x.reshape(tokens, d_model), ln_gain, ln_bias, w_q, w_k, w_v, w_o, jnp.transpose(b_query, (1, 0, 2)), jnp.transpose(b_value, (1, 0, 2)), b_attn_out, w_fc1, b_fc1, w_fc2, b_fc2, w_router, w_exp_in, b_exp_in, w_exp_out, b_exp_out)
        return result.reshape(1, tokens, d_model)

    in_specs = (P(('dp', 'ep'), None, None), P(('dp', 'ep')), P(('dp', 'ep'), None, None), P(), P(), P(None, None, 'tp', None), P(None, 'tp', None), P(None, None, 'tp', None), P(None, None, 'tp', None), P(None, 'tp', None), P(None, 'tp', None, None), P(), P(None, 'tp'), P('tp'), P('tp', None), P(), P(), P('ep', None, 'tp'), P('ep', 'tp'), P('ep', 'tp', None), P('ep', None))
    return jax.shard_map(local_fn, mesh=mesh, in_specs=in_specs, out_specs=P(('dp', 'ep'), None, None), check_vma=False)
```
